8 devices in a mesh: dp: 1 (over z), tp2: 2 (over y), tp: 4 (over x, core).
Axes of the slice: x: 2, y: 2, z: 1, core: 2. Of those that a mesh axis runs over, the one named last changes fastest.
Arguments:
- hidden: bfloat16 [1024, 2048], P('dp')
- w_gate: bfloat16 [2048, 8192], P(None, ('tp2', 'tp'))
- w_up: bfloat16 [2048, 8192], P(None, ('tp2', 'tp'))
- w_down: bfloat16 [8192, 2048], P(('tp2', 'tp'))
- norm_gain: float32 [2048], replicated
- w_vocab: bfloat16 [2048, 128256], P(None, ('tp2', 'tp'))
- temperature: float32 [1024], P('dp')
- target_ids: int32 [1024], P('dp')
Outputs:
- output 1: float32 [1024], P('dp')
- output 2: float32 [1024], P('dp')
- output 3: float32 [1024], P('dp')
- output 4: bfloat16 [1024, 128256], P('dp', ('tp2', 'tp'))
All inputs are finite; a program needn't handle non-finite values.
Results may differ from the reference program's by a relative error of at most 0.00345951.
Values are sent between devices in bfloat16 or wider.
A program may use at most 1 GiB of HBM per device.

```python
import jax
import jax.numpy as jnp
from jax import lax

BATCH_ROWS = 1024
D_MODEL = 2048
D_FF = 8192
VOCAB_SIZE = 128256
ROW_BLOCK = 8
NORM_EPS = 1e-6


def setup_inputs(seed: int = 0, part: int = 0) -> dict:
    base_key = jax.random.key(seed)
    part_key = jax.random.fold_in(base_key, part)
    shared = jax.random.split(base_key, 6)
    own_keys = jax.random.split(part_key, 3)
    hidden = jax.random.normal(own_keys[0], (BATCH_ROWS, D_MODEL), jnp.float32)
    w_gate = jax.random.normal(shared[0], (D_MODEL, D_FF), jnp.float32) * D_MODEL ** -0.5
    w_up = jax.random.normal(shared[1], (D_MODEL, D_FF), jnp.float32) * D_MODEL ** -0.5
    w_down = jax.random.normal(shared[2], (D_FF, D_MODEL), jnp.float32) * (2.0 * D_FF ** -0.5)
    norm_gain = jax.random.uniform(shared[3], (D_MODEL,), jnp.float32, 0.5, 1.5)
    col_scale = jnp.exp(0.3 * jax.random.normal(shared[4], (1, VOCAB_SIZE), jnp.float32))
    w_vocab = jax.random.normal(shared[5], (D_MODEL, VOCAB_SIZE), jnp.float32) * D_MODEL ** -0.5 * col_scale
    temperature = jax.random.uniform(own_keys[1], (BATCH_ROWS,), jnp.float32, 0.5, 2.0)
    target_ids = jax.random.randint(own_keys[2], (BATCH_ROWS,), 0, VOCAB_SIZE, jnp.int32)
    return {
        'hidden': hidden.astype(jnp.bfloat16),
        'w_gate': w_gate.astype(jnp.bfloat16),
        'w_up': w_up.astype(jnp.bfloat16),
        'w_down': w_down.astype(jnp.bfloat16),
        'norm_gain': norm_gain,
        'w_vocab': w_vocab.astype(jnp.bfloat16),
        'temperature': temperature,
        'target_ids': target_ids,
    }


def reference(hidden, w_gate, w_up, w_down, norm_gain, w_vocab, temperature, target_ids):
    gate_pre = jnp.dot(hidden, w_gate, preferred_element_type=jnp.float32)
    up_pre = jnp.dot(hidden, w_up, preferred_element_type=jnp.float32)
    hidden_act = (jax.nn.silu(gate_pre) * up_pre).astype(jnp.bfloat16)
    mlp_out = jnp.dot(hidden_act, w_down, preferred_element_type=jnp.float32).astype(jnp.bfloat16)
    resid_sum = hidden.astype(jnp.float32) + mlp_out.astype(jnp.float32)
    inv_rms = lax.rsqrt(jnp.mean(resid_sum * resid_sum, axis=-1, keepdims=True) + NORM_EPS)
    normed = (norm_gain * resid_sum * inv_rms).astype(jnp.bfloat16)
    num_blocks = BATCH_ROWS // ROW_BLOCK

    def head_block(block_in):
        block_x, block_temp, block_ids = block_in
        logits = jnp.dot(block_x, w_vocab, preferred_element_type=jnp.float32) / block_temp[:, None]
        row_max = jnp.max(logits, axis=-1, keepdims=True)
        shifted = jnp.exp(logits - row_max)
        sum_exp = jnp.sum(shifted, axis=-1)
        log_norm = row_max[:, 0] + jnp.log(sum_exp)
        mean_logit = jnp.sum(shifted * logits, axis=-1) / sum_exp
        target_logit = jnp.take_along_axis(logits, block_ids[:, None], axis=-1)[:, 0]
        logprobs = (logits - log_norm[:, None]).astype(jnp.bfloat16)
        return log_norm, log_norm - mean_logit, target_logit - log_norm, logprobs

    log_norm, entropy, target_logp, logprobs = lax.map(
        head_block,
        (normed.reshape(num_blocks, ROW_BLOCK, D_MODEL),
         temperature.reshape(num_blocks, ROW_BLOCK),
         target_ids.reshape(num_blocks, ROW_BLOCK)))
    return (log_norm.reshape(BATCH_ROWS), entropy.reshape(BATCH_ROWS),
            target_logp.reshape(BATCH_ROWS), logprobs.reshape(BATCH_ROWS, VOCAB_SIZE))
```

```python
import functools

import jax
import jax.numpy as jnp
from jax import lax
from jax.experimental import pallas as pl
from jax.experimental.pallas import tpu as pltpu
from jax.sharding import PartitionSpec as P

NORM_EPS = 1e-6
VM = pltpu.VMEM
MESH = pl.DeviceIdType.MESH
V = 16032
R = 512
BV = 1024
NT = V // BV
REM = V - NT * BV
SB = 512
NB = 3
MIB = 2 ** 20


def head_tile(w_ref, x_ref, l_ref, st_ref, row0, bv, inv_t, ids, fin=None):
    off = 0
    while off < bv:
        sb = min(SB, bv - off)
        rows = pl.ds(row0 + off, sb)
        if fin is not None:
            stage, log_norm = fin
            stage[pl.ds(off, sb), :] = (l_ref[rows, :] - log_norm).astype(jnp.bfloat16)
        logits = lax.dot_general(w_ref[pl.ds(off, sb), :], x_ref[...], (((1,), (1,)), ((), ())),
                                 preferred_element_type=jnp.float32) * inv_t
        l_ref[rows, :] = logits
        l3 = logits.reshape(sb // 8, 8, R)
        m_old = st_ref[0]
        m_new = jnp.maximum(m_old, jnp.max(l3, axis=0))
        scale = jnp.exp(m_old - m_new)
        e = jnp.exp(l3 - m_new[None])
        pos = lax.broadcasted_iota(jnp.int32, (sb // 8, 8, R), 0) * 8 + lax.broadcasted_iota(jnp.int32, (sb // 8, 8, R), 1)
        hit = pos == (ids - (row0 + off))[None]
        st_ref[0] = m_new
        st_ref[1] = st_ref[1] * scale + jnp.sum(e, axis=0)
        st_ref[2] = st_ref[2] * scale + jnp.sum(e * l3, axis=0)
        st_ref[3] = st_ref[3] + jnp.sum(jnp.where(hit, l3, 0.0), axis=0)
        off += sb


def init_stats(st_ref):
    st_ref[0] = jnp.full((8, R), -3.0e38, jnp.float32)
    st_ref[1] = jnp.zeros((8, R), jnp.float32)
    st_ref[2] = jnp.zeros((8, R), jnp.float32)
    st_ref[3] = jnp.zeros((8, R), jnp.float32)


def reduce_stats(st_ref, out_ref):
    m = jnp.max(st_ref[0], axis=0, keepdims=True)
    scale = jnp.exp(st_ref[0] - m)
    out_ref[0:1, :] = m
    out_ref[1:2, :] = jnp.sum(st_ref[1] * scale, axis=0, keepdims=True)
    out_ref[2:3, :] = jnp.sum(st_ref[2] * scale, axis=0, keepdims=True)
    out_ref[3:4, :] = jnp.sum(st_ref[3], axis=0, keepdims=True)
    out_ref[4:8, :] = jnp.zeros((4, R), jnp.float32)


def w_copy(wt_ref, wbuf, sems, tile, size):
    slot = lax.rem(tile, NB) if not isinstance(tile, int) else tile % NB
    return pltpu.make_async_copy(wt_ref.at[pl.ds(tile * BV, size)], wbuf.at[slot, pl.ds(0, size)], sems.at[slot])


def w_start(wt_ref, wbuf, sems, tile):
    @pl.when(tile < NT)
    def _():
        w_copy(wt_ref, wbuf, sems, tile, BV).start()

    @pl.when(tile == NT)
    def _():
        w_copy(wt_ref, wbuf, sems, tile, REM).start()


def head_kernel(half, last_half, *refs):
    if last_half:
        (x_ref, wt_ref, t_ref, ids_ref, res_ref, l_in, o_ref, l_ref, stat_ref,
         wbuf, st_ref, wsem, stage, osem) = refs
    else:
        x_ref, wt_ref, t_ref, ids_ref, l_ref, stat_ref, wbuf, st_ref, wsem = refs
    for t in range(NB - 1):
        w_copy(wt_ref, wbuf, wsem, t, BV).start()
    init_stats(st_ref)
    me = lax.axis_index('tp2') * 4 + lax.axis_index('tp')
    inv_t = 1.0 / t_ref[:, half * R:(half + 1) * R]
    ids = ids_ref[:, half * R:(half + 1) * R] - me * V
    x = x_ref.at[pl.ds(half * R, R)]

    def out_copy(tile, size):
        slot = lax.rem(tile, 2) if not isinstance(tile, int) else tile % 2
        return pltpu.make_async_copy(stage.at[slot, pl.ds(0, size)],
                                     o_ref.at[pl.ds(tile * BV, size), pl.ds((1 - half) * R, R)], osem.at[slot])

    def step(tile, size):
        slot = lax.rem(tile, NB) if not isinstance(tile, int) else tile % NB
        w_copy(wt_ref, wbuf, wsem, tile, size).wait()
        if not isinstance(tile, int):
            w_start(wt_ref, wbuf, wsem, tile + NB - 1)
        fin = None
        if last_half:
            oslot = lax.rem(tile, 2) if not isinstance(tile, int) else tile % 2
            if isinstance(tile, int):
                out_copy(tile - 2, BV).wait()
            else:
                @pl.when(tile >= 2)
                def _():
                    out_copy(tile - 2, BV).wait()
            fin = (stage.at[oslot], res_ref[0:1, :])
        row0 = tile * BV if isinstance(tile, int) else pl.multiple_of(tile * BV, BV)
        head_tile(wbuf.at[slot], x, l_ref, st_ref, row0, size, inv_t, ids, fin)
        if last_half:
            out_copy(tile, size).start()

    def body(i, _):
        step(i, BV)
        return 0

    lax.fori_loop(0, NT, body, 0)
    step(NT, REM)
    reduce_stats(st_ref, stat_ref)
    if last_half:
        out_copy(NT - 1, BV).wait()
        out_copy(NT, REM).wait()


def exchange_kernel(s_ref, res_ref, box, send_sem, recv_sem):
    a, b = lax.axis_index('tp2'), lax.axis_index('tp')
    bar = pltpu.get_barrier_semaphore()
    peers = [(i, j) for i in range(2) for j in range(4) if (i, j) != (0, 0)]

    def peer(d):
        return {'tp2': lax.rem(a + d[0], 2), 'tp': lax.rem(b + d[1], 4)}

    for d in peers:
        pl.semaphore_signal(bar, inc=1, device_id=peer(d), device_id_type=MESH)
    pl.semaphore_wait(bar, 7)
    copies = []
    for n, d in enumerate(peers):
        c = pltpu.make_async_remote_copy(s_ref, box.at[n], send_sem.at[n], recv_sem.at[n],
                                         device_id=peer(d), device_id_type=MESH)
        c.start()
        copies.append(c)
    for c in copies:
        c.wait()
    m = s_ref[0:1, :]
    for n in range(7):
        m = jnp.maximum(m, box[n, 0:1, :])
    k = jnp.exp(s_ref[0:1, :] - m)
    s, q, t = s_ref[1:2, :] * k, s_ref[2:3, :] * k, s_ref[3:4, :]
    for n in range(7):
        k = jnp.exp(box[n, 0:1, :] - m)
        s += box[n, 1:2, :] * k
        q += box[n, 2:3, :] * k
        t += box[n, 3:4, :]
    log_norm = m + jnp.log(s)
    res_ref[0:1, :] = log_norm
    res_ref[1:2, :] = log_norm - q / s
    res_ref[2:3, :] = t - log_norm
    res_ref[3:8, :] = jnp.zeros((5, R), jnp.float32)


def finish_kernel(l_ref, r0_ref, r1_ref, o_in, o_ref, ln_ref, en_ref, tl_ref, stage, osem):
    for half, r in ((0, r0_ref), (1, r1_ref)):
        cols = slice(half * R, (half + 1) * R)
        ln_ref[:, cols] = r[0:1, :]
        en_ref[:, cols] = r[1:2, :]
        tl_ref[:, cols] = r[2:3, :]
    log_norm = r1_ref[0:1, :]

    def out_copy(tile, size):
        slot = lax.rem(tile, 4) if not isinstance(tile, int) else tile % 4
        return pltpu.make_async_copy(stage.at[slot, pl.ds(0, size)],
                                     o_ref.at[pl.ds(tile * BV, size), pl.ds(R, R)], osem.at[slot])

    def step(tile, size):
        slot = lax.rem(tile, 4) if not isinstance(tile, int) else tile % 4
        if isinstance(tile, int):
            out_copy(tile - 4, BV).wait()
        else:
            @pl.when(tile >= 4)
            def _():
                out_copy(tile - 4, BV).wait()
        row0 = tile * BV if isinstance(tile, int) else pl.multiple_of(tile * BV, BV)
        stage[slot, 0:size, :] = (l_ref[pl.ds(row0, size), :] - log_norm).astype(jnp.bfloat16)
        out_copy(tile, size).start()

    def body(i, _):
        step(i, BV)
        return 0

    lax.fori_loop(0, NT, body, 0)
    step(NT, REM)
    for t in range(NT - 3, NT):
        out_copy(t, BV).wait()
    out_copy(NT, REM).wait()


def vspec():
    return pl.BlockSpec(memory_space=VM)


def aspec():
    return pl.BlockSpec(memory_space=pl.ANY)


def in_vmem(x):
    return pltpu.with_memory_space_constraint(x, VM)


def params(limit, **kw):
    return pltpu.CompilerParams(has_side_effects=True, vmem_limit_bytes=limit, **kw)


def head_call(half, x, wt, temp, ids, res=None, logits=None):
    last = res is not None
    l_type = VM((V, R), jnp.float32)
    stat_type = jax.ShapeDtypeStruct((8, R), jnp.float32)
    scratch = [VM((NB, BV, 2048), jnp.bfloat16), VM((4, 8, R), jnp.float32), pltpu.SemaphoreType.DMA((NB,))]
    if last:
        args = (x, wt, temp, ids, res, in_vmem(logits))
        in_specs = [vspec(), aspec(), vspec(), vspec(), vspec(), vspec()]
        out_shape = (jax.ShapeDtypeStruct((V, 2 * R), jnp.bfloat16), l_type, stat_type)
        out_specs = (aspec(), vspec(), vspec())
        scratch += [VM((2, BV, R), jnp.bfloat16), pltpu.SemaphoreType.DMA((2,))]
        alias = {5: 1}
    else:
        args = (x, wt, temp, ids)
        in_specs = [vspec(), aspec(), vspec(), vspec()]
        out_shape = (l_type, stat_type)
        out_specs = (vspec(), vspec())
        alias = {}
    return pl.pallas_call(
        functools.partial(head_kernel, half, last), out_shape=out_shape, in_specs=in_specs, out_specs=out_specs,
        scratch_shapes=scratch, input_output_aliases=alias, name='head%d' % half, compiler_params=params(24 * MIB),
        cost_estimate=pl.CostEstimate(flops=2 * V * R * 2048, bytes_accessed=V * 4096, transcendentals=V * R))(*args)


def exchange_call(stats, cid):
    return pl.pallas_call(
        exchange_kernel, out_shape=jax.ShapeDtypeStruct((8, R), jnp.float32), in_specs=[vspec()], out_specs=vspec(),
        scratch_shapes=[VM((7, 8, R), jnp.float32), pltpu.SemaphoreType.DMA((7,)), pltpu.SemaphoreType.DMA((7,))],
        name='exchange%d' % cid, compiler_params=params(8 * MIB, collective_id=cid))(stats)


def finish_call(logits, r0, r1, out):
    row = jax.ShapeDtypeStruct((1, 2 * R), jnp.float32)
    return pl.pallas_call(
        finish_kernel, out_shape=(jax.ShapeDtypeStruct((V, 2 * R), jnp.bfloat16), row, row, row),
        in_specs=[vspec(), vspec(), vspec(), aspec()], out_specs=(aspec(), vspec(), vspec(), vspec()),
        scratch_shapes=[VM((4, BV, R), jnp.bfloat16), pltpu.SemaphoreType.DMA((4,))],
        input_output_aliases={3: 0}, name='finish', compiler_params=params(12 * MIB))(in_vmem(logits), r0, r1, out)


def solution(mesh):
    model_axes = ('tp2', 'tp')

    def local_step(hidden, w_gate, w_up, w_down, norm_gain, w_vocab, temperature, target_ids):
        gate_pre = jnp.dot(hidden, w_gate, preferred_element_type=jnp.float32)
        up_pre = jnp.dot(hidden, w_up, preferred_element_type=jnp.float32)
        hidden_act = (jax.nn.silu(gate_pre) * up_pre).astype(jnp.bfloat16)
        part_out = jnp.dot(hidden_act, w_down, preferred_element_type=jnp.float32).astype(jnp.bfloat16)
        mlp_out = lax.psum(part_out, model_axes)
        resid_sum = hidden.astype(jnp.float32) + mlp_out.astype(jnp.float32)
        inv_rms = lax.rsqrt(jnp.mean(resid_sum * resid_sum, axis=-1, keepdims=True) + NORM_EPS)
        x = (norm_gain * resid_sum * inv_rms).astype(jnp.bfloat16)
        temp = temperature.reshape(1, 2 * R)
        ids = target_ids.reshape(1, 2 * R)
        wt = w_vocab.T
        l0, s0 = head_call(0, x, wt, temp, ids)
        r0 = exchange_call(s0, 1)
        out, l1, s1 = head_call(1, x, wt, temp, ids, r0, l0)
        r1 = exchange_call(s1, 2)
        out, ln, en, tl = finish_call(l1, r0, r1, out)
        return ln.reshape(-1), en.reshape(-1), tl.reshape(-1), out.T

    return jax.shard_map(
        local_step, mesh=mesh,
        in_specs=(P('dp', None), P(None, model_axes), P(None, model_axes), P(model_axes, None),
                  P(None), P(None, model_axes), P('dp'), P('dp')),
        out_specs=(P('dp'), P('dp'), P('dp'), P('dp', model_axes)),
        check_vma=False)
```

```python
import functools

import jax
import jax.numpy as jnp
from jax import lax
from jax.experimental import pallas as pl
from jax.experimental.pallas import tpu as pltpu
from jax.sharding import PartitionSpec as P

NORM_EPS = 1e-6
VM = pltpu.VMEM
MESH = pl.DeviceIdType.MESH
V = 16032
R = 512
BV = 1024
NT = V // BV
REM = V - NT * BV
SB = 256
SLICE = 128
NB = 3
MIB = 2 ** 20
LIMIT = 26 * MIB


def block_stats(l_ref, st_ref, row0, sb, ids, valid=None):
    for c in range(0, R, 128):
        lanes = slice(c, c + 128)
        m_old, s_old, q_old, t_old = (st_ref[n, :, lanes] for n in range(4))
        m, s, q, t = m_old, s_old, q_old, t_old
        for r in range(0, sb, SLICE):
            n = min(SLICE, sb - r) // 8
            l3 = l_ref[pl.ds(row0 + r, n * 8), lanes].reshape(n, 8, 128)
            m_new = jnp.maximum(m, jnp.max(l3, axis=0))
            scale = jnp.exp(m - m_new)
            e = jnp.exp(l3 - m_new[None])
            shape = (n, 8, 128)
            pos = lax.broadcasted_iota(jnp.int32, shape, 0) * 8 + lax.broadcasted_iota(jnp.int32, shape, 1)
            hit = pos == (ids[:, lanes] - (row0 + r - SB))[None]
            s = s * scale + jnp.sum(e, axis=0)
            q = q * scale + jnp.sum(e * l3, axis=0)
            t = t + jnp.sum(jnp.where(hit, l3, 0.0), axis=0)
            m = m_new
        if valid is not None:
            m, s = jnp.where(valid, m, m_old), jnp.where(valid, s, s_old)
            q, t = jnp.where(valid, q, q_old), jnp.where(valid, t, t_old)
        st_ref[0, :, lanes], st_ref[1, :, lanes], st_ref[2, :, lanes], st_ref[3, :, lanes] = m, s, q, t


def head_tile(w_ref, x_ref, l_ref, st_ref, row0, bv, inv_t, ids, fin=None, valid=None):
    off, prev = 0, SB
    while off < bv:
        sb = min(SB, bv - off)
        rows = pl.ds(row0 + SB + off, sb)
        if fin is not None:
            stage, log_norm = fin
            stage[pl.ds(off, sb), :] = (l_ref[rows, :] - log_norm).astype(jnp.bfloat16)
        logits = lax.dot_general(w_ref[pl.ds(off, sb), :], x_ref[...], (((1,), (1,)), ((), ())),
                                 preferred_element_type=jnp.float32) * inv_t
        block_stats(l_ref, st_ref, row0 + SB + off - prev, prev, ids, valid if off == 0 else None)
        l_ref[rows, :] = logits
        off, prev = off + sb, sb
    return prev


def init_stats(st_ref):
    st_ref[0] = jnp.full((8, R), -3.0e38, jnp.float32)
    st_ref[1] = jnp.zeros((8, R), jnp.float32)
    st_ref[2] = jnp.zeros((8, R), jnp.float32)
    st_ref[3] = jnp.zeros((8, R), jnp.float32)


def reduce_stats(st_ref, out_ref):
    m = jnp.max(st_ref[0], axis=0, keepdims=True)
    scale = jnp.exp(st_ref[0] - m)
    out_ref[0:1, :] = m
    out_ref[1:2, :] = jnp.sum(st_ref[1] * scale, axis=0, keepdims=True)
    out_ref[2:3, :] = jnp.sum(st_ref[2] * scale, axis=0, keepdims=True)
    out_ref[3:4, :] = jnp.sum(st_ref[3], axis=0, keepdims=True)
    out_ref[4:8, :] = jnp.zeros((4, R), jnp.float32)


def w_copy(wt_ref, wbuf, sems, tile, size):
    slot = lax.rem(tile, NB) if not isinstance(tile, int) else tile % NB
    return pltpu.make_async_copy(wt_ref.at[pl.ds(tile * BV, size)], wbuf.at[slot, pl.ds(0, size)], sems.at[slot])


def w_start(wt_ref, wbuf, sems, tile):
    @pl.when(tile < NT)
    def _():
        w_copy(wt_ref, wbuf, sems, tile, BV).start()

    @pl.when(tile == NT)
    def _():
        w_copy(wt_ref, wbuf, sems, tile, REM).start()


def head_kernel(half, last_half, *refs):
    if last_half:
        (x_ref, wt_ref, t_ref, ids_ref, res_ref, l_in, o_ref, l_ref, stat_ref,
         wbuf, st_ref, wsem, stage, osem) = refs
    else:
        x_ref, wt_ref, t_ref, ids_ref, l_ref, stat_ref, wbuf, st_ref, wsem = refs
    for t in range(NB - 1):
        w_copy(wt_ref, wbuf, wsem, t, BV).start()
    init_stats(st_ref)
    me = lax.axis_index('tp2') * 4 + lax.axis_index('tp')
    inv_t = 1.0 / t_ref[:, half * R:(half + 1) * R]
    ids = ids_ref[:, half * R:(half + 1) * R] - me * V
    x = x_ref.at[pl.ds(half * R, R)]

    def out_copy(tile, size):
        slot = lax.rem(tile, 2) if not isinstance(tile, int) else tile % 2
        return pltpu.make_async_copy(stage.at[slot, pl.ds(0, size)],
                                     o_ref.at[pl.ds(tile * BV, size), pl.ds((1 - half) * R, R)], osem.at[slot])

    def step(tile, size):
        slot = lax.rem(tile, NB) if not isinstance(tile, int) else tile % NB
        w_copy(wt_ref, wbuf, wsem, tile, size).wait()
        if not isinstance(tile, int):
            w_start(wt_ref, wbuf, wsem, tile + NB - 1)
        fin = None
        if last_half:
            oslot = lax.rem(tile, 2) if not isinstance(tile, int) else tile % 2
            if isinstance(tile, int):
                out_copy(tile - 2, BV).wait()
            else:
                @pl.when(tile >= 2)
                def _():
                    out_copy(tile - 2, BV).wait()
            fin = (stage.at[oslot], res_ref[0:1, :])
        row0 = tile * BV if isinstance(tile, int) else pl.multiple_of(tile * BV, BV)
        valid = None if isinstance(tile, int) else tile > 0
        prev = head_tile(wbuf.at[slot], x, l_ref, st_ref, row0, size, inv_t, ids, fin, valid)
        if isinstance(tile, int):
            block_stats(l_ref, st_ref, row0 + SB + size - prev, prev, ids)
        if last_half:
            out_copy(tile, size).start()

    def body(i, _):
        step(i, BV)
        return 0

    lax.fori_loop(0, NT, body, 0)
    step(NT, REM)
    reduce_stats(st_ref, stat_ref)
    if last_half:
        out_copy(NT - 1, BV).wait()
        out_copy(NT, REM).wait()


def exchange_kernel(s_ref, res_ref, box, send_sem, recv_sem):
    a, b = lax.axis_index('tp2'), lax.axis_index('tp')
    bar = pltpu.get_barrier_semaphore()
    peers = [(i, j) for i in range(2) for j in range(4) if (i, j) != (0, 0)]

    def peer(d):
        return {'tp2': lax.rem(a + d[0], 2), 'tp': lax.rem(b + d[1], 4)}

    for d in peers:
        pl.semaphore_signal(bar, inc=1, device_id=peer(d), device_id_type=MESH)
    pl.semaphore_wait(bar, 7)
    copies = []
    for n, d in enumerate(peers):
        c = pltpu.make_async_remote_copy(s_ref, box.at[n], send_sem.at[n], recv_sem.at[n],
                                         device_id=peer(d), device_id_type=MESH)
        c.start()
        copies.append(c)
    for c in copies:
        c.wait()
    m = s_ref[0:1, :]
    for n in range(7):
        m = jnp.maximum(m, box[n, 0:1, :])
    k = jnp.exp(s_ref[0:1, :] - m)
    s, q, t = s_ref[1:2, :] * k, s_ref[2:3, :] * k, s_ref[3:4, :]
    for n in range(7):
        k = jnp.exp(box[n, 0:1, :] - m)
        s += box[n, 1:2, :] * k
        q += box[n, 2:3, :] * k
        t += box[n, 3:4, :]
    log_norm = m + jnp.log(s)
    res_ref[0:1, :] = log_norm
    res_ref[1:2, :] = log_norm - q / s
    res_ref[2:3, :] = t - log_norm
    res_ref[3:8, :] = jnp.zeros((5, R), jnp.float32)


def finish_kernel(l_ref, r0_ref, r1_ref, o_in, o_ref, ln_ref, en_ref, tl_ref, stage, osem):
    for half, r in ((0, r0_ref), (1, r1_ref)):
        cols = slice(half * R, (half + 1) * R)
        ln_ref[:, cols] = r[0:1, :]
        en_ref[:, cols] = r[1:2, :]
        tl_ref[:, cols] = r[2:3, :]
    log_norm = r1_ref[0:1, :]

    def out_copy(tile, size):
        slot = lax.rem(tile, 4) if not isinstance(tile, int) else tile % 4
        return pltpu.make_async_copy(stage.at[slot, pl.ds(0, size)],
                                     o_ref.at[pl.ds(tile * BV, size), pl.ds(R, R)], osem.at[slot])

    def step(tile, size):
        slot = lax.rem(tile, 4) if not isinstance(tile, int) else tile % 4
        if isinstance(tile, int):
            out_copy(tile - 4, BV).wait()
        else:
            @pl.when(tile >= 4)
            def _():
                out_copy(tile - 4, BV).wait()
        row0 = tile * BV if isinstance(tile, int) else pl.multiple_of(tile * BV, BV)
        stage[slot, 0:size, :] = (l_ref[pl.ds(row0 + SB, size), :] - log_norm).astype(jnp.bfloat16)
        out_copy(tile, size).start()

    def body(i, _):
        step(i, BV)
        return 0

    lax.fori_loop(0, NT, body, 0)
    step(NT, REM)
    for t in range(NT - 3, NT):
        out_copy(t, BV).wait()
    out_copy(NT, REM).wait()


def vspec():
    return pl.BlockSpec(memory_space=VM)


def aspec():
    return pl.BlockSpec(memory_space=pl.ANY)


def in_vmem(x):
    return pltpu.with_memory_space_constraint(x, VM)


def params(limit, **kw):
    return pltpu.CompilerParams(has_side_effects=True, vmem_limit_bytes=limit, **kw)


def head_call(half, x, wt, temp, ids, res=None, logits=None):
    last = res is not None
    l_type = VM((V + SB, R), jnp.float32)
    stat_type = jax.ShapeDtypeStruct((8, R), jnp.float32)
    scratch = [VM((NB, BV, 2048), jnp.bfloat16), VM((4, 8, R), jnp.float32), pltpu.SemaphoreType.DMA((NB,))]
    if last:
        args = (x, wt, temp, ids, res, in_vmem(logits))
        in_specs = [vspec(), aspec(), vspec(), vspec(), vspec(), vspec()]
        out_shape = (jax.ShapeDtypeStruct((V, 2 * R), jnp.bfloat16), l_type, stat_type)
        out_specs = (aspec(), vspec(), vspec())
        scratch += [VM((2, BV, R), jnp.bfloat16), pltpu.SemaphoreType.DMA((2,))]
        alias = {5: 1}
    else:
        args = (x, wt, temp, ids)
        in_specs = [vspec(), aspec(), vspec(), vspec()]
        out_shape = (l_type, stat_type)
        out_specs = (vspec(), vspec())
        alias = {}
    return pl.pallas_call(
        functools.partial(head_kernel, half, last), out_shape=out_shape, in_specs=in_specs, out_specs=out_specs,
        scratch_shapes=scratch, input_output_aliases=alias, name='head%d' % half, compiler_params=params(LIMIT),
        cost_estimate=pl.CostEstimate(flops=2 * V * R * 2048, bytes_accessed=V * 4096, transcendentals=V * R))(*args)


def exchange_call(stats, cid):
    return pl.pallas_call(
        exchange_kernel, out_shape=jax.ShapeDtypeStruct((8, R), jnp.float32), in_specs=[vspec()], out_specs=vspec(),
        scratch_shapes=[VM((7, 8, R), jnp.float32), pltpu.SemaphoreType.DMA((7,)), pltpu.SemaphoreType.DMA((7,))],
        name='exchange%d' % cid, compiler_params=params(LIMIT, collective_id=cid))(stats)


def finish_call(logits, r0, r1, out):
    row = jax.ShapeDtypeStruct((1, 2 * R), jnp.float32)
    return pl.pallas_call(
        finish_kernel, out_shape=(jax.ShapeDtypeStruct((V, 2 * R), jnp.bfloat16), row, row, row),
        in_specs=[vspec(), vspec(), vspec(), aspec()], out_specs=(aspec(), vspec(), vspec(), vspec()),
        scratch_shapes=[VM((4, BV, R), jnp.bfloat16), pltpu.SemaphoreType.DMA((4,))],
        input_output_aliases={3: 0}, name='finish', compiler_params=params(LIMIT))(in_vmem(logits), r0, r1, out)


def solution(mesh):
    model_axes = ('tp2', 'tp')

    def local_step(hidden, w_gate, w_up, w_down, norm_gain, w_vocab, temperature, target_ids):
        gate_pre = jnp.dot(hidden, w_gate, preferred_element_type=jnp.float32)
        up_pre = jnp.dot(hidden, w_up, preferred_element_type=jnp.float32)
        hidden_act = (jax.nn.silu(gate_pre) * up_pre).astype(jnp.bfloat16)
        part_out = jnp.dot(hidden_act, w_down, preferred_element_type=jnp.float32).astype(jnp.bfloat16)
        mlp_out = lax.psum(part_out, model_axes)
        resid_sum = hidden.astype(jnp.float32) + mlp_out.astype(jnp.float32)
        inv_rms = lax.rsqrt(jnp.mean(resid_sum * resid_sum, axis=-1, keepdims=True) + NORM_EPS)
        x = (norm_gain * resid_sum * inv_rms).astype(jnp.bfloat16)
        temp = temperature.reshape(1, 2 * R)
        ids = target_ids.reshape(1, 2 * R)
        wt = w_vocab.T
        l0, s0 = head_call(0, x, wt, temp, ids)
        r0 = exchange_call(s0, 1)
        out, l1, s1 = head_call(1, x, wt, temp, ids, r0, l0)
        r1 = exchange_call(s1, 2)
        out, ln, en, tl = finish_call(l1, r0, r1, out)
        return ln.reshape(-1), en.reshape(-1), tl.reshape(-1), out.T

    return jax.shard_map(
        local_step, mesh=mesh,
        in_specs=(P('dp', None), P(None, model_axes), P(None, model_axes), P(model_axes, None),
                  P(None), P(None, model_axes), P('dp'), P('dp')),
        out_specs=(P('dp'), P('dp'), P('dp'), P('dp', model_axes)),
        check_vma=False)
```

```python
import functools

import jax
import jax.numpy as jnp
from jax import lax
from jax.experimental import pallas as pl
from jax.experimental.pallas import tpu as pltpu
from jax.sharding import PartitionSpec as P

NORM_EPS = 1e-6
VM = pltpu.VMEM
MESH = pl.DeviceIdType.MESH
V = 16032
R = 512
BV = 1024
NT = V // BV
REM = V - NT * BV
SB = 256
SLICE = 128
NB = 3
CH = 256
NQ = 4
MIB = 2 ** 20
FIRST_LIMIT = 31 * MIB
LIMIT = 26 * MIB


def block_stats(l_ref, st_ref, row0, sb, ids, valid=None):
    for c in range(0, R, 128):
        lanes = slice(c, c + 128)
        m_old, s_old, q_old, t_old = (st_ref[n, :, lanes] for n in range(4))
        m, s, q, t = m_old, s_old, q_old, t_old
        for r in range(0, sb, SLICE):
            n = min(SLICE, sb - r) // 8
            l3 = l_ref[pl.ds(row0 + r, n * 8), lanes].reshape(n, 8, 128)
            m_new = jnp.maximum(m, jnp.max(l3, axis=0))
            scale = jnp.exp(m - m_new)
            e = jnp.exp(l3 - m_new[None])
            shape = (n, 8, 128)
            pos = lax.broadcasted_iota(jnp.int32, shape, 0) * 8 + lax.broadcasted_iota(jnp.int32, shape, 1)
            hit = pos == (ids[:, lanes] - (row0 + r - SB))[None]
            s = s * scale + jnp.sum(e, axis=0)
            q = q * scale + jnp.sum(e * l3, axis=0)
            t = t + jnp.sum(jnp.where(hit, l3, 0.0), axis=0)
            m = m_new
        if valid is not None:
            m, s = jnp.where(valid, m, m_old), jnp.where(valid, s, s_old)
            q, t = jnp.where(valid, q, q_old), jnp.where(valid, t, t_old)
        st_ref[0, :, lanes], st_ref[1, :, lanes], st_ref[2, :, lanes], st_ref[3, :, lanes] = m, s, q, t


def head_tile(w_ref, x_ref, l_ref, st_ref, row0, bv, inv_t, ids, fin=None, valid=None):
    off, prev = 0, SB
    while off < bv:
        sb = min(SB, bv - off)
        rows = pl.ds(row0 + SB + off, sb)
        if fin is not None:
            stage, log_norm = fin
            stage[pl.ds(off, sb), :] = (l_ref[rows, :] - log_norm).astype(jnp.bfloat16)
        logits = lax.dot_general(w_ref[pl.ds(off, sb), :], x_ref[...], (((1,), (1,)), ((), ())),
                                 preferred_element_type=jnp.float32) * inv_t
        block_stats(l_ref, st_ref, row0 + SB + off - prev, prev, ids, valid if off == 0 else None)
        l_ref[rows, :] = logits
        off, prev = off + sb, sb
    return prev


def init_stats(st_ref):
    st_ref[0] = jnp.full((8, R), -3.0e38, jnp.float32)
    st_ref[1] = jnp.zeros((8, R), jnp.float32)
    st_ref[2] = jnp.zeros((8, R), jnp.float32)
    st_ref[3] = jnp.zeros((8, R), jnp.float32)


def reduce_stats(st_ref, out_ref):
    m = jnp.max(st_ref[0], axis=0, keepdims=True)
    scale = jnp.exp(st_ref[0] - m)
    out_ref[0:1, :] = m
    out_ref[1:2, :] = jnp.sum(st_ref[1] * scale, axis=0, keepdims=True)
    out_ref[2:3, :] = jnp.sum(st_ref[2] * scale, axis=0, keepdims=True)
    out_ref[3:4, :] = jnp.sum(st_ref[3], axis=0, keepdims=True)
    out_ref[4:8, :] = jnp.zeros((4, R), jnp.float32)


def w_copy(wt_ref, wbuf, sems, tile, size):
    slot = lax.rem(tile, NB) if not isinstance(tile, int) else tile % NB
    return pltpu.make_async_copy(wt_ref.at[pl.ds(tile * BV, size)], wbuf.at[slot, pl.ds(0, size)], sems.at[slot])


def w_start(wt_ref, wbuf, sems, tile):
    @pl.when(tile < NT)
    def _():
        w_copy(wt_ref, wbuf, sems, tile, BV).start()

    @pl.when(tile == NT)
    def _():
        w_copy(wt_ref, wbuf, sems, tile, REM).start()


def head_loop(wt_ref, wbuf, wsem, x_ref, l_ref, st_ref, inv_t, ids, out=None, hooks=()):
    if out is not None:
        o_ref, col0, stage, osem, log_norm = out

    def out_copy(tile, size):
        slot = lax.rem(tile, 2) if not isinstance(tile, int) else tile % 2
        return pltpu.make_async_copy(stage.at[slot, pl.ds(0, size)],
                                     o_ref.at[pl.ds(tile * BV, size), pl.ds(col0, R)], osem.at[slot])

    def step(tile, size):
        last = isinstance(tile, int)
        slot = tile % NB if last else lax.rem(tile, NB)
        w_copy(wt_ref, wbuf, wsem, tile, size).wait()
        if not last:
            w_start(wt_ref, wbuf, wsem, tile + NB - 1)
        fin = None
        if out is not None:
            if last:
                out_copy(tile - 2, BV).wait()
            else:
                @pl.when(tile >= 2)
                def _():
                    out_copy(tile - 2, BV).wait()
            fin = (stage.at[tile % 2 if last else lax.rem(tile, 2)], log_norm)
        row0 = tile * BV if last else pl.multiple_of(tile * BV, BV)
        prev = head_tile(wbuf.at[slot], x_ref, l_ref, st_ref, row0, size, inv_t, ids, fin, None if last else tile > 0)
        if last:
            block_stats(l_ref, st_ref, row0 + SB + size - prev, prev, ids)
        if out is not None:
            out_copy(tile, size).start()

    def body(i, _):
        for at, hook in hooks:
            pl.when(i == at)(hook)
        step(i, BV)
        return 0

    lax.fori_loop(0, NT, body, 0)
    step(NT, REM)
    if out is not None:
        out_copy(NT - 1, BV).wait()
        out_copy(NT, REM).wait()


def place():
    a, b = lax.axis_index('tp2'), lax.axis_index('tp')
    return a, b // 2, b % 2


PEERS = [(i, j) for i in range(2) for j in range(4) if (i, j) != (0, 0)]


def peer(d):
    a, b = lax.axis_index('tp2'), lax.axis_index('tp')
    return {'tp2': (a + d[0]) % 2, 'tp': (b + d[1]) % 4}


def barrier():
    bar = pltpu.get_barrier_semaphore()
    for d in PEERS:
        pl.semaphore_signal(bar, inc=1, device_id=peer(d), device_id_type=MESH)
    pl.semaphore_wait(bar, 7)


def exchange(s_ref, res_ref, box, send_sem, recv_sem):
    copies = []
    for n, d in enumerate(PEERS):
        c = pltpu.make_async_remote_copy(s_ref, box.at[n], send_sem.at[n], recv_sem.at[n],
                                         device_id=peer(d), device_id_type=MESH)
        c.start()
        copies.append(c)
    for c in copies:
        c.wait()
    m = s_ref[0:1, :]
    for n in range(7):
        m = jnp.maximum(m, box[n, 0:1, :])
    k = jnp.exp(s_ref[0:1, :] - m)
    s, q, t = s_ref[1:2, :] * k, s_ref[2:3, :] * k, s_ref[3:4, :]
    for n in range(7):
        k = jnp.exp(box[n, 0:1, :] - m)
        s += box[n, 1:2, :] * k
        q += box[n, 2:3, :] * k
        t += box[n, 3:4, :]
    log_norm = m + jnp.log(s)
    res_ref[0:1, :] = log_norm
    res_ref[1:2, :] = log_norm - q / s
    res_ref[2:3, :] = t - log_norm
    res_ref[3:8, :] = jnp.zeros((5, R), jnp.float32)


def exchange_kernel(s_ref, res_ref, box, send_sem, recv_sem):
    barrier()
    exchange(s_ref, res_ref, box, send_sem, recv_sem)


def first_kernel(h_ref, wg_ref, wu_ref, wd_ref, gain_ref, wt_ref, t_ref, ids_ref,
                 l_ref, x1_ref, res_ref,
                 wbuf, hbuf, hres, act, part, drecv, rbuf, x, st_ref, sbuf, box,
                 wsem, msem, hsem, hrsem, dsem, rsem, gsem, fsem, xsem, esem):
    y, xx, c = place()
    g = 2 * y + xx
    me = lax.axis_index('tp2') * 4 + lax.axis_index('tp')
    half = CH // 2
    own = half // 4

    def weights(n):
        src = (wg_ref, wu_ref)[n]
        return [pltpu.make_async_copy(src.at[pl.ds(k * 1024, 1024)], wbuf.at[n, :, pl.ds(k * 1024, 1024)],
                                      msem.at[2 * n + k]) for k in range(2)]

    down = pltpu.make_async_copy(wd_ref, wbuf.at[2], msem.at[4])

    def h_copy(q):
        return pltpu.make_async_copy(h_ref.at[pl.ds(q * CH, CH)], hbuf, hsem)

    def own_rows(q):
        return pl.ds(q * CH + c * half + g * own, own)

    def res_copy(q):
        return pltpu.make_async_copy(h_ref.at[own_rows(q)], hres.at[q], hrsem.at[q])

    def chip(d):
        cx = (xx + d % 2) % 2
        cy = (y + d // 2) % 2
        return cy, cx, {'tp2': cy, 'tp': 2 * cx + c}

    sibling = {'tp2': y, 'tp': 2 * xx + (c + 1) % 2}

    def d_copy(q):
        return pltpu.make_async_remote_copy(part.at[q, pl.ds(((c + 1) % 2) * half, half)], drecv.at[q],
                                            dsem.at[0, q], dsem.at[1, q], device_id=sibling, device_id_type=MESH)

    def r_copy(q, d):
        cy, cx, dev = chip(d)
        return pltpu.make_async_remote_copy(part.at[q, pl.ds(c * half + (2 * cy + cx) * own, own)], rbuf.at[q, d - 1],
                                            rsem.at[0, q, d - 1], rsem.at[1, q, d - 1], device_id=dev,
                                            device_id_type=MESH)

    def g_copy(q, d):
        return pltpu.make_async_remote_copy(x.at[own_rows(q)], x.at[own_rows(q)],
                                            gsem.at[0, q, d - 1], gsem.at[1, q, d - 1], device_id=chip(d)[2],
                                            device_id_type=MESH)

    def f_copy(q):
        rows = pl.ds(q * CH + c * half, half)
        return pltpu.make_async_remote_copy(x.at[rows], x.at[rows], fsem.at[0, q], fsem.at[1, q],
                                            device_id=sibling, device_id_type=MESH)

    def pair_sum(q):
        d_copy(q).wait()
        rows = pl.ds(c * half, half)
        part[q, rows, :] = (part[q, rows, :].astype(jnp.float32) + drecv[q].astype(jnp.float32)).astype(jnp.bfloat16)
        for d in (3, 1, 2):
            r_copy(q, d).start()

    def total(q):
        for d in (1, 2, 3):
            r_copy(q, d).wait()
        res_copy(q).wait()
        mlp = part[q, pl.ds(c * half + g * own, own), :].astype(jnp.float32)
        for d in range(3):
            mlp += rbuf[q, d].astype(jnp.float32)
        resid = hres[q].astype(jnp.float32) + mlp.astype(jnp.bfloat16).astype(jnp.float32)
        inv_rms = lax.rsqrt(jnp.mean(resid * resid, axis=-1, keepdims=True) + NORM_EPS)
        x[own_rows(q), :] = (gain_ref[...] * resid * inv_rms).astype(jnp.bfloat16)
        for d in (3, 1, 2):
            g_copy(q, d).start()

    def gathered(q):
        for d in (1, 2, 3):
            g_copy(q, d).wait()
        f_copy(q).start()

    h_copy(0).start()
    for n in range(2):
        for cp in weights(n):
            cp.start()
    down.start()
    for q in range(NQ):
        res_copy(q).start()
    init_stats(st_ref)
    barrier()

    def mlp(q, _):
        h_copy(q).wait()

        @pl.when(q == 0)
        def _():
            for n in range(2):
                for cp in weights(n):
                    cp.wait()
        h = hbuf
        for n in range(0, 1024, 512):
            pre = [jnp.dot(h[:, 0:1024], wbuf[k, :, n:n + 512], preferred_element_type=jnp.float32)
                   + jnp.dot(h[:, 1024:2048], wbuf[k, :, 1024 + n:1536 + n], preferred_element_type=jnp.float32)
                   for k in range(2)]
            act[:, n:n + 512] = (jax.nn.silu(pre[0]) * pre[1]).astype(jnp.bfloat16)

        @pl.when(q + 1 < NQ)
        def _():
            h_copy(q + 1).start()

        @pl.when(q == NQ - 1)
        def _():
            for t in range(NB - 1):
                w_copy(wt_ref, wbuf, wsem, t, BV).start()

        @pl.when(q == 0)
        def _():
            down.wait()
        for n in range(0, 2048, 512):
            part[q, :, n:n + 512] = jnp.dot(act[...], wbuf[2, :, n:n + 512],
                                            preferred_element_type=jnp.float32).astype(jnp.bfloat16)
        d_copy(q).start()

        @pl.when((q >= 1) & (q <= NQ // 2))
        def _():
            pair_sum(q - 1)
        return 0

    lax.fori_loop(0, NQ, mlp, 0)
    first = range(NQ // 2)
    second = range(NQ // 2, NQ)
    for q in first:
        total(q)
    for q in second:
        pair_sum(q)
    for q in first:
        gathered(q)
    for q in first:
        f_copy(q).wait()

    def x1_copy():
        return pltpu.make_async_copy(x.at[pl.ds(R, R)], x1_ref, xsem)

    def last_rows():
        for q in second:
            f_copy(q).wait()
        x1_copy().start()

    n2 = len(second)
    hooks = [(2 + 2 * k, functools.partial(total, q)) for k, q in enumerate(second)]
    hooks += [(3 + 2 * n2 + 2 * k, functools.partial(gathered, q)) for k, q in enumerate(second)]
    hooks += [(4 + 4 * n2, last_rows)]
    ids = ids_ref[:, 0:R] - me * V
    head_loop(wt_ref, wbuf, wsem, x.at[pl.ds(0, R)], l_ref, st_ref, 1.0 / t_ref[:, 0:R], ids, hooks=hooks)
    reduce_stats(st_ref, sbuf)
    x1_copy().wait()
    exchange(sbuf, res_ref, box, esem.at[0], esem.at[1])


def second_kernel(x_ref, wt_ref, t_ref, ids_ref, res_ref, l_in, o_ref, l_ref, stat_ref,
                  wbuf, st_ref, wsem, stage, osem):
    for t in range(NB - 1):
        w_copy(wt_ref, wbuf, wsem, t, BV).start()
    init_stats(st_ref)
    me = lax.axis_index('tp2') * 4 + lax.axis_index('tp')
    ids = ids_ref[:, R:2 * R] - me * V
    head_loop(wt_ref, wbuf, wsem, x_ref, l_ref, st_ref, 1.0 / t_ref[:, R:2 * R], ids,
              out=(o_ref, 0, stage, osem, res_ref[0:1, :]))
    reduce_stats(st_ref, stat_ref)


def finish_kernel(l_ref, r0_ref, r1_ref, o_in, o_ref, ln_ref, en_ref, tl_ref, stage, osem):
    for half, r in ((0, r0_ref), (1, r1_ref)):
        cols = slice(half * R, (half + 1) * R)
        ln_ref[:, cols] = r[0:1, :]
        en_ref[:, cols] = r[1:2, :]
        tl_ref[:, cols] = r[2:3, :]
    log_norm = r1_ref[0:1, :]

    def out_copy(tile, size):
        slot = lax.rem(tile, 4) if not isinstance(tile, int) else tile % 4
        return pltpu.make_async_copy(stage.at[slot, pl.ds(0, size)],
                                     o_ref.at[pl.ds(tile * BV, size), pl.ds(R, R)], osem.at[slot])

    def step(tile, size):
        slot = lax.rem(tile, 4) if not isinstance(tile, int) else tile % 4
        if isinstance(tile, int):
            out_copy(tile - 4, BV).wait()
        else:
            @pl.when(tile >= 4)
            def _():
                out_copy(tile - 4, BV).wait()
        row0 = tile * BV if isinstance(tile, int) else pl.multiple_of(tile * BV, BV)
        stage[slot, 0:size, :] = (l_ref[pl.ds(row0 + SB, size), :] - log_norm).astype(jnp.bfloat16)
        out_copy(tile, size).start()

    def body(i, _):
        step(i, BV)
        return 0

    lax.fori_loop(0, NT, body, 0)
    step(NT, REM)
    for t in range(NT - 3, NT):
        out_copy(t, BV).wait()
    out_copy(NT, REM).wait()


def vspec():
    return pl.BlockSpec(memory_space=VM)


def aspec():
    return pl.BlockSpec(memory_space=pl.ANY)


def in_vmem(x):
    return pltpu.with_memory_space_constraint(x, VM)


def params(limit, **kw):
    return pltpu.CompilerParams(has_side_effects=True, vmem_limit_bytes=limit, **kw)


L_TYPE = VM((V + SB, R), jnp.float32)
HEAD_COST = pl.CostEstimate(flops=2 * V * R * 2048, bytes_accessed=V * 4096, transcendentals=V * R)


def first_call(hidden, w_gate, w_up, w_down, gain, wt, temp, ids):
    dma = pltpu.SemaphoreType.DMA
    half, own = CH // 2, CH // 8
    return pl.pallas_call(
        first_kernel,
        out_shape=(L_TYPE, jax.ShapeDtypeStruct((R, 2048), jnp.bfloat16), jax.ShapeDtypeStruct((8, R), jnp.float32)),
        in_specs=[aspec()] * 4 + [vspec(), aspec(), vspec(), vspec()], out_specs=(vspec(), aspec(), vspec()),
        scratch_shapes=[
            VM((NB, BV, 2048), jnp.bfloat16), VM((CH, 2048), jnp.bfloat16), VM((NQ, own, 2048), jnp.bfloat16),
            VM((CH, 1024), jnp.bfloat16), VM((NQ, CH, 2048), jnp.bfloat16), VM((NQ, half, 2048), jnp.bfloat16),
            VM((NQ, 3, own, 2048), jnp.bfloat16), VM((2 * R, 2048), jnp.bfloat16), VM((4, 8, R), jnp.float32),
            VM((8, R), jnp.float32), VM((7, 8, R), jnp.float32),
            dma((NB,)), dma((5,)), dma, dma((NQ,)), dma((2, NQ)), dma((2, NQ, 3)), dma((2, NQ, 3)), dma((2, NQ)),
            dma, dma((2, 7))],
        name='first', cost_estimate=HEAD_COST,
        compiler_params=params(FIRST_LIMIT, collective_id=0))(hidden, w_gate, w_up, w_down, gain, wt, temp, ids)


def second_call(x1, wt, temp, ids, res, logits):
    return pl.pallas_call(
        second_kernel,
        out_shape=(jax.ShapeDtypeStruct((V, 2 * R), jnp.bfloat16), L_TYPE, jax.ShapeDtypeStruct((8, R), jnp.float32)),
        in_specs=[vspec(), aspec(), vspec(), vspec(), vspec(), vspec()], out_specs=(aspec(), vspec(), vspec()),
        scratch_shapes=[VM((NB, BV, 2048), jnp.bfloat16), VM((4, 8, R), jnp.float32), pltpu.SemaphoreType.DMA((NB,)),
                        VM((2, BV, R), jnp.bfloat16), pltpu.SemaphoreType.DMA((2,))],
        input_output_aliases={5: 1}, name='second', cost_estimate=HEAD_COST,
        compiler_params=params(LIMIT))(x1, wt, temp, ids, res, in_vmem(logits))


def exchange_call(stats, cid):
    return pl.pallas_call(
        exchange_kernel, out_shape=jax.ShapeDtypeStruct((8, R), jnp.float32), in_specs=[vspec()], out_specs=vspec(),
        scratch_shapes=[VM((7, 8, R), jnp.float32), pltpu.SemaphoreType.DMA((7,)), pltpu.SemaphoreType.DMA((7,))],
        name='exchange%d' % cid, compiler_params=params(LIMIT, collective_id=cid))(stats)


def finish_call(logits, r0, r1, out):
    row = jax.ShapeDtypeStruct((1, 2 * R), jnp.float32)
    return pl.pallas_call(
        finish_kernel, out_shape=(jax.ShapeDtypeStruct((V, 2 * R), jnp.bfloat16), row, row, row),
        in_specs=[vspec(), vspec(), vspec(), aspec()], out_specs=(aspec(), vspec(), vspec(), vspec()),
        scratch_shapes=[VM((4, BV, R), jnp.bfloat16), pltpu.SemaphoreType.DMA((4,))],
        input_output_aliases={3: 0}, name='finish', compiler_params=params(LIMIT))(in_vmem(logits), r0, r1, out)


def solution(mesh):
    model_axes = ('tp2', 'tp')

    def local_step(hidden, w_gate, w_up, w_down, norm_gain, w_vocab, temperature, target_ids):
        temp = temperature.reshape(1, 2 * R)
        ids = target_ids.reshape(1, 2 * R)
        wt = w_vocab.T
        l0, x1, r0 = first_call(hidden, w_gate, w_up, w_down, norm_gain.reshape(1, -1), wt, temp, ids)
        out, l1, s1 = second_call(x1, wt, temp, ids, r0, l0)
        r1 = exchange_call(s1, 2)
        out, ln, en, tl = finish_call(l1, r0, r1, out)
        return ln.reshape(-1), en.reshape(-1), tl.reshape(-1), out.T

    return jax.shard_map(
        local_step, mesh=mesh,
        in_specs=(P('dp', None), P(None, model_axes), P(None, model_axes), P(model_axes, None),
                  P(None), P(None, model_axes), P('dp'), P('dp')),
        out_specs=(P('dp'), P('dp'), P('dp'), P('dp', model_axes)),
        check_vma=False)
```

```python
import functools

import jax
import jax.numpy as jnp
from jax import lax
from jax.experimental import pallas as pl
from jax.experimental.pallas import tpu as pltpu
from jax.sharding import PartitionSpec as P

NORM_EPS = 1e-6
VM = pltpu.VMEM
MESH = pl.DeviceIdType.MESH
V = 16032
R = 512
BV = 1024
NT = V // BV
REM = V - NT * BV
SB = 512
SLICE = 128
NB = 3
CH = 256
NQ = 4
MIB = 2 ** 20
LOG2E = 1.4426950408889634
FIRST_LIMIT = 31 * MIB
LIMIT = 26 * MIB


def block_stats(l_ref, st_ref, row0, vocab0, sb, scale2, ids, valid=None):
    for c in range(0, R, 128):
        lanes = slice(c, c + 128)
        a = scale2[:, lanes]
        m_old, s_old, q_old, t_old = (st_ref[n, :, lanes] for n in range(4))
        m, s, q, t = m_old, s_old, q_old, t_old
        rel = ids[:, lanes] - vocab0 - lax.broadcasted_iota(jnp.int32, (8, 128), 0)
        for r in range(0, sb, SLICE):
            n = min(SLICE, sb - r) // 8
            l3 = l_ref[pl.ds(row0 + r, n * 8), lanes].reshape(n, 8, 128)
            m_new = jnp.maximum(m, jnp.max(l3, axis=0))
            scale = jnp.exp2((m - m_new) * a)
            e = jnp.exp2((l3 - m_new[None]) * a[None])
            s = s * scale + jnp.sum(e, axis=0)
            q = q * scale + jnp.sum(e * l3, axis=0)
            for j in range(n):
                t = jnp.where(rel == r + 8 * j, l3[j], t)
            m = m_new
        if valid is not None:
            m, s = jnp.where(valid, m, m_old), jnp.where(valid, s, s_old)
            q, t = jnp.where(valid, q, q_old), jnp.where(valid, t, t_old)
        st_ref[0, :, lanes], st_ref[1, :, lanes], st_ref[2, :, lanes], st_ref[3, :, lanes] = m, s, q, t


def head_tile(w_ref, x_ref, l_ref, st_ref, row0, bv, prev0, scale2, ids, fin=None, valid=None):
    for off in range(0, BV, SB):
        block_stats(l_ref, st_ref, prev0 + off, prev0 + off, SB, scale2, ids, valid)
        sb = min(SB, bv - off)
        if sb <= 0:
            continue
        rows = pl.ds(row0 + off, sb)
        if fin is not None:
            stage, inv_t, log_norm = fin
            stage[pl.ds(off, sb), :] = (l_ref[rows, :] * inv_t - log_norm).astype(jnp.bfloat16)
        l_ref[rows, :] = lax.dot_general(w_ref[pl.ds(off, sb), :], x_ref[...], (((1,), (1,)), ((), ())),
                                         preferred_element_type=jnp.float32)


def init_stats(st_ref):
    st_ref[0] = jnp.full((8, R), -3.0e38, jnp.float32)
    st_ref[1] = jnp.zeros((8, R), jnp.float32)
    st_ref[2] = jnp.zeros((8, R), jnp.float32)
    st_ref[3] = jnp.zeros((8, R), jnp.float32)


def reduce_stats(st_ref, out_ref, inv_t):
    m = jnp.max(st_ref[0], axis=0, keepdims=True)
    scale = jnp.exp2((st_ref[0] - m) * (inv_t * LOG2E))
    out_ref[0:1, :] = m * inv_t
    out_ref[1:2, :] = jnp.sum(st_ref[1] * scale, axis=0, keepdims=True)
    out_ref[2:3, :] = jnp.sum(st_ref[2] * scale, axis=0, keepdims=True) * inv_t
    out_ref[3:4, :] = jnp.sum(st_ref[3], axis=0, keepdims=True) * inv_t
    out_ref[4:8, :] = jnp.zeros((4, R), jnp.float32)


def w_copy(wt_ref, wbuf, sems, tile, size):
    slot = lax.rem(tile, NB) if not isinstance(tile, int) else tile % NB
    return pltpu.make_async_copy(wt_ref.at[pl.ds(tile * BV, size)], wbuf.at[slot, pl.ds(0, size)], sems.at[slot])


def w_start(wt_ref, wbuf, sems, tile):
    @pl.when(tile < NT)
    def _():
        w_copy(wt_ref, wbuf, sems, tile, BV).start()

    @pl.when(tile == NT)
    def _():
        w_copy(wt_ref, wbuf, sems, tile, REM).start()


def head_loop(wt_ref, wbuf, wsem, x_ref, l_ref, st_ref, inv_t, ids, out=None, hooks=()):
    scale2 = inv_t * LOG2E
    if out is not None:
        o_ref, col0, stage, osem, out_inv_t, log_norm = out

    def out_copy(tile, size):
        slot = lax.rem(tile, 2) if not isinstance(tile, int) else tile % 2
        return pltpu.make_async_copy(stage.at[slot, pl.ds(0, size)],
                                     o_ref.at[pl.ds(tile * BV, size), pl.ds(col0, R)], osem.at[slot])

    def step(tile, size):
        last = isinstance(tile, int)
        slot = tile % NB if last else lax.rem(tile, NB)
        w_copy(wt_ref, wbuf, wsem, tile, size).wait()
        if not last:
            w_start(wt_ref, wbuf, wsem, tile + NB - 1)
        fin = None
        if out is not None:
            if last:
                out_copy(tile - 2, BV).wait()
            else:
                @pl.when(tile >= 2)
                def _():
                    out_copy(tile - 2, BV).wait()
            fin = (stage.at[tile % 2 if last else lax.rem(tile, 2)], out_inv_t, log_norm)
        row0 = tile * BV if last else pl.multiple_of(tile * BV, BV)
        prev0 = row0 - BV if last else pl.multiple_of(jnp.maximum(row0 - BV, 0), BV)
        head_tile(wbuf.at[slot], x_ref, l_ref, st_ref, row0, size, prev0, scale2, ids, fin, None if last else tile > 0)
        if last:
            block_stats(l_ref, st_ref, row0, row0, size, scale2, ids)
        if out is not None:
            out_copy(tile, size).start()

    def body(i, _):
        for at, hook in hooks:
            pl.when(i == at)(hook)
        step(i, BV)
        return 0

    lax.fori_loop(0, NT, body, 0)
    step(NT, REM)
    if out is not None:
        out_copy(NT - 1, BV).wait()
        out_copy(NT, REM).wait()


def place():
    a, b = lax.axis_index('tp2'), lax.axis_index('tp')
    return a, b // 2, b % 2


PEERS = [(i, j) for i in range(2) for j in range(4) if (i, j) != (0, 0)]


def peer(d):
    a, b = lax.axis_index('tp2'), lax.axis_index('tp')
    return {'tp2': (a + d[0]) % 2, 'tp': (b + d[1]) % 4}


def barrier():
    bar = pltpu.get_barrier_semaphore()
    for d in PEERS:
        pl.semaphore_signal(bar, inc=1, device_id=peer(d), device_id_type=MESH)
    pl.semaphore_wait(bar, 7)


def exchange(s_ref, res_ref, box, send_sem, recv_sem):
    copies = []
    for n, d in enumerate(PEERS):
        c = pltpu.make_async_remote_copy(s_ref, box.at[n], send_sem.at[n], recv_sem.at[n],
                                         device_id=peer(d), device_id_type=MESH)
        c.start()
        copies.append(c)
    for c in copies:
        c.wait()
    m = s_ref[0:1, :]
    for n in range(7):
        m = jnp.maximum(m, box[n, 0:1, :])
    k = jnp.exp(s_ref[0:1, :] - m)
    s, q, t = s_ref[1:2, :] * k, s_ref[2:3, :] * k, s_ref[3:4, :]
    for n in range(7):
        k = jnp.exp(box[n, 0:1, :] - m)
        s += box[n, 1:2, :] * k
        q += box[n, 2:3, :] * k
        t += box[n, 3:4, :]
    log_norm = m + jnp.log(s)
    res_ref[0:1, :] = log_norm
    res_ref[1:2, :] = log_norm - q / s
    res_ref[2:3, :] = t - log_norm
    res_ref[3:8, :] = jnp.zeros((5, R), jnp.float32)


def exchange_kernel(s_ref, res_ref, box, send_sem, recv_sem):
    barrier()
    exchange(s_ref, res_ref, box, send_sem, recv_sem)


def first_kernel(h_ref, wg_ref, wu_ref, wd_ref, gain_ref, wt_ref, t_ref, ids_ref,
                 l_ref, x1_ref, res_ref,
                 wbuf, hbuf, hres, act, part, drecv, rbuf, x, st_ref, sbuf, box,
                 wsem, msem, hsem, hrsem, dsem, rsem, gsem, fsem, xsem, esem):
    y, xx, c = place()
    g = 2 * y + xx
    me = lax.axis_index('tp2') * 4 + lax.axis_index('tp')
    half = CH // 2
    own = half // 4

    def weights(n):
        src = (wg_ref, wu_ref)[n]
        return [pltpu.make_async_copy(src.at[pl.ds(k * 1024, 1024)], wbuf.at[n, :, pl.ds(k * 1024, 1024)],
                                      msem.at[2 * n + k]) for k in range(2)]

    down = pltpu.make_async_copy(wd_ref, wbuf.at[2], msem.at[4])

    def h_copy(q):
        return pltpu.make_async_copy(h_ref.at[pl.ds(q * CH, CH)], hbuf, hsem)

    def own_rows(q):
        return pl.ds(q * CH + c * half + g * own, own)

    def res_copy(q):
        return pltpu.make_async_copy(h_ref.at[own_rows(q)], hres.at[q], hrsem.at[q])

    def chip(d):
        cx = (xx + d % 2) % 2
        cy = (y + d // 2) % 2
        return cy, cx, {'tp2': cy, 'tp': 2 * cx + c}

    sibling = {'tp2': y, 'tp': 2 * xx + (c + 1) % 2}

    def d_copy(q):
        return pltpu.make_async_remote_copy(part.at[q, pl.ds(((c + 1) % 2) * half, half)], drecv.at[q],
                                            dsem.at[0, q], dsem.at[1, q], device_id=sibling, device_id_type=MESH)

    def r_copy(q, d):
        cy, cx, dev = chip(d)
        return pltpu.make_async_remote_copy(part.at[q, pl.ds(c * half + (2 * cy + cx) * own, own)], rbuf.at[q, d - 1],
                                            rsem.at[0, q, d - 1], rsem.at[1, q, d - 1], device_id=dev,
                                            device_id_type=MESH)

    def g_copy(q, d):
        return pltpu.make_async_remote_copy(x.at[own_rows(q)], x.at[own_rows(q)],
                                            gsem.at[0, q, d - 1], gsem.at[1, q, d - 1], device_id=chip(d)[2],
                                            device_id_type=MESH)

    def f_copy(q):
        rows = pl.ds(q * CH + c * half, half)
        return pltpu.make_async_remote_copy(x.at[rows], x.at[rows], fsem.at[0, q], fsem.at[1, q],
                                            device_id=sibling, device_id_type=MESH)

    def pair_sum(q):
        d_copy(q).wait()
        rows = pl.ds(c * half, half)
        part[q, rows, :] = (part[q, rows, :].astype(jnp.float32) + drecv[q].astype(jnp.float32)).astype(jnp.bfloat16)
        for d in (3, 1, 2):
            r_copy(q, d).start()

    def total(q):
        for d in (1, 2, 3):
            r_copy(q, d).wait()
        res_copy(q).wait()
        mlp = part[q, pl.ds(c * half + g * own, own), :].astype(jnp.float32)
        for d in range(3):
            mlp += rbuf[q, d].astype(jnp.float32)
        resid = hres[q].astype(jnp.float32) + mlp.astype(jnp.bfloat16).astype(jnp.float32)
        inv_rms = lax.rsqrt(jnp.mean(resid * resid, axis=-1, keepdims=True) + NORM_EPS)
        x[own_rows(q), :] = (gain_ref[...] * resid * inv_rms).astype(jnp.bfloat16)
        for d in (3, 1, 2):
            g_copy(q, d).start()

    def gathered(q):
        for d in (1, 2, 3):
            g_copy(q, d).wait()
        f_copy(q).start()

    h_copy(0).start()
    for n in range(2):
        for cp in weights(n):
            cp.start()
    down.start()
    for q in range(NQ):
        res_copy(q).start()
    init_stats(st_ref)
    barrier()

    def mlp(q, _):
        h_copy(q).wait()

        @pl.when(q == 0)
        def _():
            for n in range(2):
                for cp in weights(n):
                    cp.wait()
        h = hbuf
        for n in range(0, 1024, 512):
            pre = [jnp.dot(h[:, 0:1024], wbuf[k, :, n:n + 512], preferred_element_type=jnp.float32)
                   + jnp.dot(h[:, 1024:2048], wbuf[k, :, 1024 + n:1536 + n], preferred_element_type=jnp.float32)
                   for k in range(2)]
            act[:, n:n + 512] = (jax.nn.silu(pre[0]) * pre[1]).astype(jnp.bfloat16)

        @pl.when(q + 1 < NQ)
        def _():
            h_copy(q + 1).start()

        @pl.when(q == NQ - 1)
        def _():
            for t in range(NB - 1):
                w_copy(wt_ref, wbuf, wsem, t, BV).start()

        @pl.when(q == 0)
        def _():
            down.wait()
        for n in range(0, 2048, 512):
            part[q, :, n:n + 512] = jnp.dot(act[...], wbuf[2, :, n:n + 512],
                                            preferred_element_type=jnp.float32).astype(jnp.bfloat16)
        d_copy(q).start()

        @pl.when((q >= 1) & (q <= NQ // 2))
        def _():
            pair_sum(q - 1)
        return 0

    lax.fori_loop(0, NQ, mlp, 0)
    first = range(NQ // 2)
    second = range(NQ // 2, NQ)
    for q in first:
        total(q)
    for q in second:
        pair_sum(q)
    for q in first:
        gathered(q)
    for q in first:
        f_copy(q).wait()

    def x1_copy():
        return pltpu.make_async_copy(x.at[pl.ds(R, R)], x1_ref, xsem)

    def last_rows():
        for q in second:
            f_copy(q).wait()
        x1_copy().start()

    n2 = len(second)
    hooks = [(2 + 2 * k, functools.partial(total, q)) for k, q in enumerate(second)]
    hooks += [(3 + 2 * n2 + 2 * k, functools.partial(gathered, q)) for k, q in enumerate(second)]
    hooks += [(4 + 4 * n2, last_rows)]
    ids = ids_ref[:, 0:R] - me * V
    head_loop(wt_ref, wbuf, wsem, x.at[pl.ds(0, R)], l_ref, st_ref, 1.0 / t_ref[:, 0:R], ids, hooks=hooks)
    reduce_stats(st_ref, sbuf, 1.0 / t_ref[:, 0:R])
    x1_copy().wait()
    exchange(sbuf, res_ref, box, esem.at[0], esem.at[1])


def second_kernel(x_ref, wt_ref, t_ref, ids_ref, res_ref, l_in, o_ref, l_ref, stat_ref,
                  wbuf, st_ref, wsem, stage, osem):
    for t in range(NB - 1):
        w_copy(wt_ref, wbuf, wsem, t, BV).start()
    init_stats(st_ref)
    me = lax.axis_index('tp2') * 4 + lax.axis_index('tp')
    ids = ids_ref[:, R:2 * R] - me * V
    head_loop(wt_ref, wbuf, wsem, x_ref, l_ref, st_ref, 1.0 / t_ref[:, R:2 * R], ids,
              out=(o_ref, 0, stage, osem, 1.0 / t_ref[:, 0:R], res_ref[0:1, :]))
    reduce_stats(st_ref, stat_ref, 1.0 / t_ref[:, R:2 * R])


def finish_kernel(l_ref, r0_ref, r1_ref, t_ref, o_in, o_ref, ln_ref, en_ref, tl_ref, stage, osem):
    for half, r in ((0, r0_ref), (1, r1_ref)):
        cols = slice(half * R, (half + 1) * R)
        ln_ref[:, cols] = r[0:1, :]
        en_ref[:, cols] = r[1:2, :]
        tl_ref[:, cols] = r[2:3, :]
    log_norm = r1_ref[0:1, :]
    inv_t = 1.0 / t_ref[:, R:2 * R]

    def out_copy(tile, size):
        slot = lax.rem(tile, 4) if not isinstance(tile, int) else tile % 4
        return pltpu.make_async_copy(stage.at[slot, pl.ds(0, size)],
                                     o_ref.at[pl.ds(tile * BV, size), pl.ds(R, R)], osem.at[slot])

    def step(tile, size):
        slot = lax.rem(tile, 4) if not isinstance(tile, int) else tile % 4
        if isinstance(tile, int):
            out_copy(tile - 4, BV).wait()
        else:
            @pl.when(tile >= 4)
            def _():
                out_copy(tile - 4, BV).wait()
        row0 = tile * BV if isinstance(tile, int) else pl.multiple_of(tile * BV, BV)
        stage[slot, 0:size, :] = (l_ref[pl.ds(row0, size), :] * inv_t - log_norm).astype(jnp.bfloat16)
        out_copy(tile, size).start()

    def body(i, _):
        step(i, BV)
        return 0

    lax.fori_loop(0, NT, body, 0)
    step(NT, REM)
    for t in range(NT - 3, NT):
        out_copy(t, BV).wait()
    out_copy(NT, REM).wait()


def vspec():
    return pl.BlockSpec(memory_space=VM)


def aspec():
    return pl.BlockSpec(memory_space=pl.ANY)


def in_vmem(x):
    return pltpu.with_memory_space_constraint(x, VM)


def params(limit, **kw):
    return pltpu.CompilerParams(has_side_effects=True, vmem_limit_bytes=limit, **kw)


L_TYPE = VM((V, R), jnp.float32)
HEAD_COST = pl.CostEstimate(flops=2 * V * R * 2048, bytes_accessed=V * 4096, transcendentals=V * R)


def first_call(hidden, w_gate, w_up, w_down, gain, wt, temp, ids):
    dma = pltpu.SemaphoreType.DMA
    half, own = CH // 2, CH // 8
    return pl.pallas_call(
        first_kernel,
        out_shape=(L_TYPE, jax.ShapeDtypeStruct((R, 2048), jnp.bfloat16), jax.ShapeDtypeStruct((8, R), jnp.float32)),
        in_specs=[aspec()] * 4 + [vspec(), aspec(), vspec(), vspec()], out_specs=(vspec(), aspec(), vspec()),
        scratch_shapes=[
            VM((NB, BV, 2048), jnp.bfloat16), VM((CH, 2048), jnp.bfloat16), VM((NQ, own, 2048), jnp.bfloat16),
            VM((CH, 1024), jnp.bfloat16), VM((NQ, CH, 2048), jnp.bfloat16), VM((NQ, half, 2048), jnp.bfloat16),
            VM((NQ, 3, own, 2048), jnp.bfloat16), VM((2 * R, 2048), jnp.bfloat16), VM((4, 8, R), jnp.float32),
            VM((8, R), jnp.float32), VM((7, 8, R), jnp.float32),
            dma((NB,)), dma((5,)), dma, dma((NQ,)), dma((2, NQ)), dma((2, NQ, 3)), dma((2, NQ, 3)), dma((2, NQ)),
            dma, dma((2, 7))],
        name='first', cost_estimate=HEAD_COST,
        compiler_params=params(FIRST_LIMIT, collective_id=0))(hidden, w_gate, w_up, w_down, gain, wt, temp, ids)


def second_call(x1, wt, temp, ids, res, logits):
    return pl.pallas_call(
        second_kernel,
        out_shape=(jax.ShapeDtypeStruct((V, 2 * R), jnp.bfloat16), L_TYPE, jax.ShapeDtypeStruct((8, R), jnp.float32)),
        in_specs=[vspec(), aspec(), vspec(), vspec(), vspec(), vspec()], out_specs=(aspec(), vspec(), vspec()),
        scratch_shapes=[VM((NB, BV, 2048), jnp.bfloat16), VM((4, 8, R), jnp.float32), pltpu.SemaphoreType.DMA((NB,)),
                        VM((2, BV, R), jnp.bfloat16), pltpu.SemaphoreType.DMA((2,))],
        input_output_aliases={5: 1}, name='second', cost_estimate=HEAD_COST,
        compiler_params=params(LIMIT))(x1, wt, temp, ids, res, in_vmem(logits))


def exchange_call(stats, cid):
    return pl.pallas_call(
        exchange_kernel, out_shape=jax.ShapeDtypeStruct((8, R), jnp.float32), in_specs=[vspec()], out_specs=vspec(),
        scratch_shapes=[VM((7, 8, R), jnp.float32), pltpu.SemaphoreType.DMA((7,)), pltpu.SemaphoreType.DMA((7,))],
        name='exchange%d' % cid, compiler_params=params(LIMIT, collective_id=cid))(stats)


def finish_call(logits, r0, r1, temp, out):
    row = jax.ShapeDtypeStruct((1, 2 * R), jnp.float32)
    return pl.pallas_call(
        finish_kernel, out_shape=(jax.ShapeDtypeStruct((V, 2 * R), jnp.bfloat16), row, row, row),
        in_specs=[vspec(), vspec(), vspec(), vspec(), aspec()], out_specs=(aspec(), vspec(), vspec(), vspec()),
        scratch_shapes=[VM((4, BV, R), jnp.bfloat16), pltpu.SemaphoreType.DMA((4,))],
        input_output_aliases={4: 0}, name='finish', compiler_params=params(LIMIT))(in_vmem(logits), r0, r1, temp, out)


def solution(mesh):
    model_axes = ('tp2', 'tp')

    def local_step(hidden, w_gate, w_up, w_down, norm_gain, w_vocab, temperature, target_ids):
        temp = temperature.reshape(1, 2 * R)
        ids = target_ids.reshape(1, 2 * R)
        wt = w_vocab.T
        l0, x1, r0 = first_call(hidden, w_gate, w_up, w_down, norm_gain.reshape(1, -1), wt, temp, ids)
        out, l1, s1 = second_call(x1, wt, temp, ids, r0, l0)
        r1 = exchange_call(s1, 2)
        out, ln, en, tl = finish_call(l1, r0, r1, temp, out)
        return ln.reshape(-1), en.reshape(-1), tl.reshape(-1), out.T

    return jax.shard_map(
        local_step, mesh=mesh,
        in_specs=(P('dp', None), P(None, model_axes), P(None, model_axes), P(model_axes, None),
                  P(None), P(None, model_axes), P('dp'), P('dp')),
        out_specs=(P('dp'), P('dp'), P('dp'), P('dp', model_axes)),
        check_vma=False)
```

```python
import functools

import jax
import jax.numpy as jnp
from jax import lax
from jax.experimental import pallas as pl
from jax.experimental.pallas import tpu as pltpu
from jax.sharding import PartitionSpec as P

NORM_EPS = 1e-6
VM = pltpu.VMEM
MESH = pl.DeviceIdType.MESH
V = 16032
R = 512
BV = 1024
NT = V // BV
REM = V - NT * BV
SB = 512
SLICE = 128
NB = 3
CH = 128
NQ = 8
LAG = 5
EARLY = 7
FV, FS = 512, 8
MIB = 2 ** 20
LOG2E = 1.4426950408889634
FIRST_LIMIT = 31 * MIB
LIMIT = 26 * MIB


def block_stats(l_ref, st_ref, row0, vocab0, sb, scale2, ids, valid=None, span=(0, R)):
    for c in range(span[0], span[1], 128):
        lanes = slice(c, c + 128)
        a = scale2[:, lanes]
        m_old, s_old, q_old, t_old = (st_ref[n, :, lanes] for n in range(4))
        m, s, q, t = m_old, s_old, q_old, t_old
        rel = ids[:, lanes] - vocab0 - lax.broadcasted_iota(jnp.int32, (8, 128), 0)
        for r in range(0, sb, SLICE):
            n = min(SLICE, sb - r) // 8
            l3 = l_ref[pl.ds(row0 + r, n * 8), lanes].reshape(n, 8, 128)
            m_new = jnp.maximum(m, jnp.max(l3, axis=0))
            scale = jnp.exp2((m - m_new) * a)
            e = jnp.exp2((l3 - m_new[None]) * a[None])
            s = s * scale + jnp.sum(e, axis=0)
            q = q * scale + jnp.sum(e * l3, axis=0)
            for j in range(n):
                t = jnp.where(rel == r + 8 * j, l3[j], t)
            m = m_new
        if valid is not None:
            m, s = jnp.where(valid, m, m_old), jnp.where(valid, s, s_old)
            q, t = jnp.where(valid, q, q_old), jnp.where(valid, t, t_old)
        st_ref[0, :, lanes], st_ref[1, :, lanes], st_ref[2, :, lanes], st_ref[3, :, lanes] = m, s, q, t


def head_tile(w_ref, x_ref, l_ref, st_ref, row0, bv, prev0, scale2, ids, fin=None, valid=None, span=(0, R)):
    for off in range(0, BV, SB):
        block_stats(l_ref, st_ref, prev0 + off, prev0 + off, SB, scale2, ids, valid, span)
        sb = min(SB, bv - off)
        if sb <= 0:
            continue
        rows = pl.ds(row0 + off, sb)
        if fin is not None:
            stage, inv_t, log_norm = fin
            stage[pl.ds(off, sb), :] = (l_ref[rows, :] * inv_t - log_norm).astype(jnp.bfloat16)
        l_ref[rows, span[0]:span[1]] = lax.dot_general(w_ref[pl.ds(off, sb), :], x_ref[span[0]:span[1], :], (((1,), (1,)), ((), ())),
                                                       preferred_element_type=jnp.float32)


def init_stats(st_ref):
    st_ref[0] = jnp.full((8, R), -3.0e38, jnp.float32)
    st_ref[1] = jnp.zeros((8, R), jnp.float32)
    st_ref[2] = jnp.zeros((8, R), jnp.float32)
    st_ref[3] = jnp.zeros((8, R), jnp.float32)


def reduce_stats(st_ref, out_ref, inv_t):
    m = jnp.max(st_ref[0], axis=0, keepdims=True)
    scale = jnp.exp2((st_ref[0] - m) * (inv_t * LOG2E))
    out_ref[0:1, :] = m * inv_t
    out_ref[1:2, :] = jnp.sum(st_ref[1] * scale, axis=0, keepdims=True)
    out_ref[2:3, :] = jnp.sum(st_ref[2] * scale, axis=0, keepdims=True) * inv_t
    out_ref[3:4, :] = jnp.sum(st_ref[3], axis=0, keepdims=True) * inv_t
    out_ref[4:8, :] = jnp.zeros((4, R), jnp.float32)


def w_copy(wt_ref, wbuf, sems, seq, size):
    slot = seq % NB if isinstance(seq, int) else lax.rem(seq, NB)
    tile = seq % (NT + 1) if isinstance(seq, int) else lax.rem(seq, NT + 1)
    return pltpu.make_async_copy(wt_ref.at[pl.ds(tile * BV, size)], wbuf.at[slot, pl.ds(0, size)], sems.at[slot])


def w_start(wt_ref, wbuf, sems, seq, end):
    @pl.when((seq < end) & (seq != NT))
    def _():
        w_copy(wt_ref, wbuf, sems, seq, BV).start()

    @pl.when(seq == NT)
    def _():
        w_copy(wt_ref, wbuf, sems, seq, REM).start()


def head_loop(wt_ref, wbuf, wsem, x_ref, l_ref, st_ref, inv_t, ids, out=None, hooks=(), first=0, count=NT + 1,
              end=NT + 1, span=(0, R)):
    scale2 = inv_t * LOG2E
    if out is not None:
        o_ref, col0, stage, osem, out_inv_t, log_norm = out

    def out_copy(tile, size):
        slot = lax.rem(tile, 2) if not isinstance(tile, int) else tile % 2
        return pltpu.make_async_copy(stage.at[slot, pl.ds(0, size)],
                                     o_ref.at[pl.ds(tile * BV, size), pl.ds(col0, R)], osem.at[slot])

    def step(seq, size):
        last = isinstance(seq, int)
        slot = seq % NB if last else lax.rem(seq, NB)
        tile = seq - (NT + 1 if first > NT else 0)
        w_copy(wt_ref, wbuf, wsem, seq, size).wait()
        w_start(wt_ref, wbuf, wsem, jnp.int32(seq + NB - 1), end)
        fin = None
        if out is not None:
            if last:
                out_copy(tile - 2, BV).wait()
            else:
                @pl.when(tile >= 2)
                def _():
                    out_copy(tile - 2, BV).wait()
            fin = (stage.at[tile % 2 if last else lax.rem(tile, 2)], out_inv_t, log_norm)
        row0 = tile * BV if last else pl.multiple_of(tile * BV, BV)
        prev0 = row0 - BV if last else pl.multiple_of(jnp.maximum(row0 - BV, 0), BV)
        head_tile(wbuf.at[slot], x_ref, l_ref, st_ref, row0, size, prev0, scale2, ids, fin,
                  None if last else seq > first, span)
        if out is not None:
            out_copy(tile, size).start()

    def body(i, _):
        for at, hook in hooks:
            pl.when(i == at)(hook)
        step(i, BV)
        return 0

    stop = min(first + count, NT) if first <= NT else first + count
    lax.fori_loop(first, stop, body, 0)
    if first <= NT < first + count:
        step(NT, REM)
        row0, size = NT * BV, REM
    else:
        row0, size = (stop - 1) % (NT + 1) * BV, BV
    block_stats(l_ref, st_ref, row0, row0, size, scale2, ids, span=span)
    if out is not None:
        out_copy(NT - 1, BV).wait()
        out_copy(NT, REM).wait()


def place():
    a, b = lax.axis_index('tp2'), lax.axis_index('tp')
    return a, b // 2, b % 2


PEERS = [(i, j) for i in range(2) for j in range(4) if (i, j) != (0, 0)]


def peer(d):
    a, b = lax.axis_index('tp2'), lax.axis_index('tp')
    return {'tp2': (a + d[0]) % 2, 'tp': (b + d[1]) % 4}


def barrier():
    bar = pltpu.get_barrier_semaphore()
    for d in PEERS:
        pl.semaphore_signal(bar, inc=1, device_id=peer(d), device_id_type=MESH)
    pl.semaphore_wait(bar, 7)


def exchange(s_ref, res_ref, box, send_sem, recv_sem):
    copies = []
    for n, d in enumerate(PEERS):
        c = pltpu.make_async_remote_copy(s_ref, box.at[n], send_sem.at[n], recv_sem.at[n],
                                         device_id=peer(d), device_id_type=MESH)
        c.start()
        copies.append(c)
    for c in copies:
        c.wait()
    m = s_ref[0:1, :]
    for n in range(7):
        m = jnp.maximum(m, box[n, 0:1, :])
    k = jnp.exp(s_ref[0:1, :] - m)
    s, q, t = s_ref[1:2, :] * k, s_ref[2:3, :] * k, s_ref[3:4, :]
    for n in range(7):
        k = jnp.exp(box[n, 0:1, :] - m)
        s += box[n, 1:2, :] * k
        q += box[n, 2:3, :] * k
        t += box[n, 3:4, :]
    log_norm = m + jnp.log(s)
    res_ref[0:1, :] = log_norm
    res_ref[1:2, :] = log_norm - q / s
    res_ref[2:3, :] = t - log_norm
    res_ref[3:8, :] = jnp.zeros((5, R), jnp.float32)


def exchange_kernel(s_ref, res_ref, box, send_sem, recv_sem):
    barrier()
    exchange(s_ref, res_ref, box, send_sem, recv_sem)


def first_kernel(h_ref, wg_ref, wu_ref, wd_ref, gain_ref, wt_ref, t_ref, ids_ref,
                 l_ref, x1_ref, res_ref,
                 wbuf, hbuf, hres, act, part, drecv, rbuf, x, st_ref, sbuf, box,
                 wsem, msem, hsem, hrsem, dsem, rsem, gsem, fsem, xsem, esem):
    y, xx, c = place()
    g = 2 * y + xx
    me = lax.axis_index('tp2') * 4 + lax.axis_index('tp')
    half = CH // 2
    own = half // 4

    def weights(n):
        src = (wg_ref, wu_ref)[n]
        return [pltpu.make_async_copy(src.at[pl.ds(k * 1024, 1024)], wbuf.at[n, :, pl.ds(k * 1024, 1024)],
                                      msem.at[2 * n + k]) for k in range(2)]

    down = pltpu.make_async_copy(wd_ref, wbuf.at[2], msem.at[4])

    def h_copy(q):
        return pltpu.make_async_copy(h_ref.at[pl.ds(q * CH, CH)], hbuf, hsem)

    def own_rows(q):
        return pl.ds(q * CH + c * half + g * own, own)

    def res_copy(q):
        return pltpu.make_async_copy(h_ref.at[own_rows(q)], hres.at[q], hrsem.at[q])

    def chip(d):
        cx = (xx + d % 2) % 2
        cy = (y + d // 2) % 2
        return cy, cx, {'tp2': cy, 'tp': 2 * cx + c}

    sibling = {'tp2': y, 'tp': 2 * xx + (c + 1) % 2}

    def d_copy(q):
        return pltpu.make_async_remote_copy(part.at[q, pl.ds(((c + 1) % 2) * half, half)], drecv.at[q],
                                            dsem.at[0, q], dsem.at[1, q], device_id=sibling, device_id_type=MESH)

    def r_copy(q, d):
        cy, cx, dev = chip(d)
        return pltpu.make_async_remote_copy(part.at[q, pl.ds(c * half + (2 * cy + cx) * own, own)], rbuf.at[q, d - 1],
                                            rsem.at[0, q, d - 1], rsem.at[1, q, d - 1], device_id=dev,
                                            device_id_type=MESH)

    def g_copy(q, d):
        return pltpu.make_async_remote_copy(x.at[own_rows(q)], x.at[own_rows(q)],
                                            gsem.at[0, q, d - 1], gsem.at[1, q, d - 1], device_id=chip(d)[2],
                                            device_id_type=MESH)

    def f_copy(q):
        rows = pl.ds(q * CH + c * half, half)
        return pltpu.make_async_remote_copy(x.at[rows], x.at[rows], fsem.at[0, q], fsem.at[1, q],
                                            device_id=sibling, device_id_type=MESH)

    def pair_sum(q):
        d_copy(q).wait()
        rows = pl.ds(c * half, half)
        part[q, rows, :] = (part[q, rows, :].astype(jnp.float32) + drecv[q].astype(jnp.float32)).astype(jnp.bfloat16)
        for d in (3, 1, 2):
            r_copy(q, d).start()

    def total(q):
        for d in (1, 2, 3):
            r_copy(q, d).wait()
        res_copy(q).wait()
        mlp = part[q, pl.ds(c * half + g * own, own), :].astype(jnp.float32)
        for d in range(3):
            mlp += rbuf[q, d].astype(jnp.float32)
        resid = hres[q].astype(jnp.float32) + mlp.astype(jnp.bfloat16).astype(jnp.float32)
        inv_rms = lax.rsqrt(jnp.mean(resid * resid, axis=-1, keepdims=True) + NORM_EPS)
        x[own_rows(q), :] = (gain_ref[...] * resid * inv_rms).astype(jnp.bfloat16)
        for d in (3, 1, 2):
            g_copy(q, d).start()

    def gathered(q):
        for d in (1, 2, 3):
            g_copy(q, d).wait()
        f_copy(q).start()

    h_copy(0).start()
    for n in range(2):
        for cp in weights(n):
            cp.start()
    down.start()
    for q in range(NQ):
        res_copy(q).start()
    init_stats(st_ref)
    barrier()

    def mlp(q, _):
        h_copy(q).wait()

        @pl.when(q == 0)
        def _():
            for n in range(2):
                for cp in weights(n):
                    cp.wait()
        h = hbuf
        for n in range(0, 1024, 512):
            pre = [jnp.dot(h[:, 0:1024], wbuf[k, :, n:n + 512], preferred_element_type=jnp.float32)
                   + jnp.dot(h[:, 1024:2048], wbuf[k, :, 1024 + n:1536 + n], preferred_element_type=jnp.float32)
                   for k in range(2)]
            act[:, n:n + 512] = (jax.nn.silu(pre[0]) * pre[1]).astype(jnp.bfloat16)

        @pl.when(q + 1 < NQ)
        def _():
            h_copy(q + 1).start()

        @pl.when(q == NQ - 1)
        def _():
            for t in range(NB - 1):
                w_copy(wt_ref, wbuf, wsem, t, BV).start()

        @pl.when(q == 0)
        def _():
            down.wait()

        @pl.when((q >= 1) & (q <= NQ // 2))
        def _():
            pair_sum(q - 1)
        for n in range(0, 2048, 512):
            part[q, :, n:n + 512] = jnp.dot(act[...], wbuf[2, :, n:n + 512],
                                            preferred_element_type=jnp.float32).astype(jnp.bfloat16)
        d_copy(q).start()

        @pl.when(q >= LAG)
        def _():
            total(q - LAG)
        return 0

    lax.fori_loop(0, NQ, mlp, 0)
    first, second, third = range(NQ // 4), range(NQ // 4, NQ // 2), range(NQ // 2, NQ)
    for q in range(NQ - LAG, NQ // 2):
        total(q)
    for q in first:
        gathered(q)
    for q in first:
        f_copy(q).wait()
    ids = ids_ref[:, 0:R] - me * V
    head = functools.partial(head_loop, wt_ref, wbuf, wsem, x.at[pl.ds(0, R)], l_ref, st_ref, 1.0 / t_ref[:, 0:R], ids,
                             end=NT + 1 + EARLY)
    head(first=0, count=EARLY, span=(0, R // 2))
    for q in second:
        gathered(q)
    for q in third:
        pair_sum(q)
    for q in second:
        f_copy(q).wait()

    def x1_copy():
        return pltpu.make_async_copy(x.at[pl.ds(R, R)], x1_ref, xsem)

    def last_rows():
        for q in third:
            f_copy(q).wait()
        x1_copy().start()

    hooks = [(EARLY + 1 + k, functools.partial(total, q)) for k, q in enumerate(third)]
    head(first=EARLY, count=NT + 1 - EARLY, hooks=hooks)
    for q in third:
        gathered(q)
    head(first=NT + 1, count=EARLY, span=(R // 2, R), hooks=[(NT + 1 + EARLY - 2, last_rows)])
    reduce_stats(st_ref, sbuf, 1.0 / t_ref[:, 0:R])
    x1_copy().wait()
    exchange(sbuf, res_ref, box, esem.at[0], esem.at[1])


def second_kernel(x_ref, wt_ref, t_ref, ids_ref, res_ref, l_in, o_ref, l_ref, stat_ref,
                  wbuf, st_ref, wsem, stage, osem):
    for t in range(NB - 1):
        w_copy(wt_ref, wbuf, wsem, t, BV).start()
    init_stats(st_ref)
    me = lax.axis_index('tp2') * 4 + lax.axis_index('tp')
    ids = ids_ref[:, R:2 * R] - me * V
    head_loop(wt_ref, wbuf, wsem, x_ref, l_ref, st_ref, 1.0 / t_ref[:, R:2 * R], ids,
              out=(o_ref, 0, stage, osem, 1.0 / t_ref[:, 0:R], res_ref[0:1, :]))
    reduce_stats(st_ref, stat_ref, 1.0 / t_ref[:, R:2 * R])


def finish_kernel(l_ref, r0_ref, r1_ref, t_ref, o_in, o_ref, ln_ref, en_ref, tl_ref, stage, osem):
    for half, r in ((0, r0_ref), (1, r1_ref)):
        cols = slice(half * R, (half + 1) * R)
        ln_ref[:, cols] = r[0:1, :]
        en_ref[:, cols] = r[1:2, :]
        tl_ref[:, cols] = r[2:3, :]
    log_norm = r1_ref[0:1, :]
    inv_t = 1.0 / t_ref[:, R:2 * R]

    def out_copy(tile, size):
        slot = tile % FS if isinstance(tile, int) else lax.rem(tile, FS)
        return pltpu.make_async_copy(stage.at[slot, pl.ds(0, size)],
                                     o_ref.at[pl.ds(tile * FV, size), pl.ds(R, R)], osem.at[slot])

    def step(tile, size):
        slot = tile % FS if isinstance(tile, int) else lax.rem(tile, FS)
        if isinstance(tile, int):
            out_copy(tile - FS, FV).wait()
        else:
            @pl.when(tile >= FS)
            def _():
                out_copy(tile - FS, FV).wait()
        row0 = tile * FV if isinstance(tile, int) else pl.multiple_of(tile * FV, FV)
        stage[slot, 0:size, :] = (l_ref[pl.ds(row0, size), :] * inv_t - log_norm).astype(jnp.bfloat16)
        out_copy(tile, size).start()

    def body(i, _):
        step(i, FV)
        return 0

    n = V // FV
    lax.fori_loop(0, n, body, 0)
    step(n, V - n * FV)
    for t in range(n + 1 - FS, n):
        out_copy(t, FV).wait()
    out_copy(n, V - n * FV).wait()


def vspec():
    return pl.BlockSpec(memory_space=VM)


def aspec():
    return pl.BlockSpec(memory_space=pl.ANY)


def in_vmem(x):
    return pltpu.with_memory_space_constraint(x, VM)


def params(limit, **kw):
    return pltpu.CompilerParams(has_side_effects=True, vmem_limit_bytes=limit, **kw)


L_TYPE = VM((V, R), jnp.float32)
HEAD_COST = pl.CostEstimate(flops=2 * V * R * 2048, bytes_accessed=V * 4096, transcendentals=V * R)


def first_call(hidden, w_gate, w_up, w_down, gain, wt, temp, ids):
    dma = pltpu.SemaphoreType.DMA
    half, own = CH // 2, CH // 8
    return pl.pallas_call(
        first_kernel,
        out_shape=(L_TYPE, jax.ShapeDtypeStruct((R, 2048), jnp.bfloat16), jax.ShapeDtypeStruct((8, R), jnp.float32)),
        in_specs=[aspec()] * 4 + [vspec(), aspec(), vspec(), vspec()], out_specs=(vspec(), aspec(), vspec()),
        scratch_shapes=[
            VM((NB, BV, 2048), jnp.bfloat16), VM((CH, 2048), jnp.bfloat16), VM((NQ, own, 2048), jnp.bfloat16),
            VM((CH, 1024), jnp.bfloat16), VM((NQ, CH, 2048), jnp.bfloat16), VM((NQ, half, 2048), jnp.bfloat16),
            VM((NQ, 3, own, 2048), jnp.bfloat16), VM((2 * R, 2048), jnp.bfloat16), VM((4, 8, R), jnp.float32),
            VM((8, R), jnp.float32), VM((7, 8, R), jnp.float32),
            dma((NB,)), dma((5,)), dma, dma((NQ,)), dma((2, NQ)), dma((2, NQ, 3)), dma((2, NQ, 3)), dma((2, NQ)),
            dma, dma((2, 7))],
        name='first', cost_estimate=HEAD_COST,
        compiler_params=params(FIRST_LIMIT, collective_id=0))(hidden, w_gate, w_up, w_down, gain, wt, temp, ids)


def second_call(x1, wt, temp, ids, res, logits):
    return pl.pallas_call(
        second_kernel,
        out_shape=(jax.ShapeDtypeStruct((V, 2 * R), jnp.bfloat16), L_TYPE, jax.ShapeDtypeStruct((8, R), jnp.float32)),
        in_specs=[vspec(), aspec(), vspec(), vspec(), vspec(), vspec()], out_specs=(aspec(), vspec(), vspec()),
        scratch_shapes=[VM((NB, BV, 2048), jnp.bfloat16), VM((4, 8, R), jnp.float32), pltpu.SemaphoreType.DMA((NB,)),
                        VM((2, BV, R), jnp.bfloat16), pltpu.SemaphoreType.DMA((2,))],
        input_output_aliases={5: 1}, name='second', cost_estimate=HEAD_COST,
        compiler_params=params(LIMIT))(x1, wt, temp, ids, res, in_vmem(logits))


def exchange_call(stats, cid):
    return pl.pallas_call(
        exchange_kernel, out_shape=jax.ShapeDtypeStruct((8, R), jnp.float32), in_specs=[vspec()], out_specs=vspec(),
        scratch_shapes=[VM((7, 8, R), jnp.float32), pltpu.SemaphoreType.DMA((7,)), pltpu.SemaphoreType.DMA((7,))],
        name='exchange%d' % cid, compiler_params=params(LIMIT, collective_id=cid))(stats)


def finish_call(logits, r0, r1, temp, out):
    row = jax.ShapeDtypeStruct((1, 2 * R), jnp.float32)
    return pl.pallas_call(
        finish_kernel, out_shape=(jax.ShapeDtypeStruct((V, 2 * R), jnp.bfloat16), row, row, row),
        in_specs=[vspec(), vspec(), vspec(), vspec(), aspec()], out_specs=(aspec(), vspec(), vspec(), vspec()),
        scratch_shapes=[VM((FS, FV, R), jnp.bfloat16), pltpu.SemaphoreType.DMA((FS,))],
        input_output_aliases={4: 0}, name='finish', compiler_params=params(LIMIT))(in_vmem(logits), r0, r1, temp, out)


def solution(mesh):
    model_axes = ('tp2', 'tp')

    def local_step(hidden, w_gate, w_up, w_down, norm_gain, w_vocab, temperature, target_ids):
        temp = temperature.reshape(1, 2 * R)
        ids = target_ids.reshape(1, 2 * R)
        wt = w_vocab.T
        l0, x1, r0 = first_call(hidden, w_gate, w_up, w_down, norm_gain.reshape(1, -1), wt, temp, ids)
        out, l1, s1 = second_call(x1, wt, temp, ids, r0, l0)
        r1 = exchange_call(s1, 2)
        out, ln, en, tl = finish_call(l1, r0, r1, temp, out)
        return ln.reshape(-1), en.reshape(-1), tl.reshape(-1), out.T

    return jax.shard_map(
        local_step, mesh=mesh,
        in_specs=(P('dp', None), P(None, model_axes), P(None, model_axes), P(model_axes, None),
                  P(None), P(None, model_axes), P('dp'), P('dp')),
        out_specs=(P('dp'), P('dp'), P('dp'), P('dp', model_axes)),
        check_vma=False)
```

```python
import functools

import jax
import jax.numpy as jnp
from jax import lax
from jax.experimental import pallas as pl
from jax.experimental.pallas import tpu as pltpu
from jax.sharding import PartitionSpec as P

NORM_EPS = 1e-6
VM = pltpu.VMEM
MESH = pl.DeviceIdType.MESH
V = 16032
R = 512
BV = 1024
NT = V // BV
REM = V - NT * BV
SB = 512
SLICE = 128
NB = 3
CH = 128
NQ = 8
LAG = 4
EARLY = 7
FV, FS = 512, 8
MIB = 2 ** 20
LOG2E = 1.4426950408889634
FIRST_LIMIT = 31 * MIB
LIMIT = 26 * MIB


def block_stats(l_ref, st_ref, row0, vocab0, sb, scale2, ids, valid=None, span=(0, R)):
    for c in range(span[0], span[1], 128):
        lanes = slice(c, c + 128)
        a = scale2[:, lanes]
        m_old, s_old, q_old, t_old = (st_ref[n, :, lanes] for n in range(4))
        m, s, q, t = m_old, s_old, q_old, t_old
        rel = ids[:, lanes] - vocab0 - lax.broadcasted_iota(jnp.int32, (8, 128), 0)
        for r in range(0, sb, SLICE):
            n = min(SLICE, sb - r) // 8
            l3 = l_ref[pl.ds(row0 + r, n * 8), lanes].reshape(n, 8, 128)
            m_new = jnp.maximum(m, jnp.max(l3, axis=0))
            scale = jnp.exp2((m - m_new) * a)
            e = jnp.exp2((l3 - m_new[None]) * a[None])
            s = s * scale + jnp.sum(e, axis=0)
            q = q * scale + jnp.sum(e * l3, axis=0)
            for j in range(n):
                t = jnp.where(rel == r + 8 * j, l3[j], t)
            m = m_new
        if valid is not None:
            m, s = jnp.where(valid, m, m_old), jnp.where(valid, s, s_old)
            q, t = jnp.where(valid, q, q_old), jnp.where(valid, t, t_old)
        st_ref[0, :, lanes], st_ref[1, :, lanes], st_ref[2, :, lanes], st_ref[3, :, lanes] = m, s, q, t


def head_tile(w_ref, x_ref, l_ref, st_ref, row0, bv, prev0, scale2, ids, fin=None, valid=None, span=(0, R)):
    def stats(off, n):
        block_stats(l_ref, st_ref, prev0 + off, prev0 + off, n, scale2, ids, valid, span)

    def dot(off, n):
        sb = min(n, bv - off)
        if sb <= 0:
            return
        rows = pl.ds(row0 + off, sb)
        if fin is not None:
            stage, inv_t, log_norm = fin
            stage[pl.ds(off, sb), :] = (l_ref[rows, :] * inv_t - log_norm).astype(jnp.bfloat16)
        l_ref[rows, span[0]:span[1]] = lax.dot_general(w_ref[pl.ds(off, sb), :], x_ref[span[0]:span[1], :],
                                                       (((1,), (1,)), ((), ())), preferred_element_type=jnp.float32)

    if fin is not None:
        dot(0, SB)
        stats(0, BV)
        dot(SB, SB)
    else:
        for off in range(0, BV, SB // 2):
            stats(off, SB // 2)
            dot(off, SB // 2)


def init_stats(st_ref):
    st_ref[0] = jnp.full((8, R), -3.0e38, jnp.float32)
    st_ref[1] = jnp.zeros((8, R), jnp.float32)
    st_ref[2] = jnp.zeros((8, R), jnp.float32)
    st_ref[3] = jnp.zeros((8, R), jnp.float32)


def reduce_stats(st_ref, out_ref, inv_t):
    m = jnp.max(st_ref[0], axis=0, keepdims=True)
    scale = jnp.exp2((st_ref[0] - m) * (inv_t * LOG2E))
    out_ref[0:1, :] = m * inv_t
    out_ref[1:2, :] = jnp.sum(st_ref[1] * scale, axis=0, keepdims=True)
    out_ref[2:3, :] = jnp.sum(st_ref[2] * scale, axis=0, keepdims=True) * inv_t
    out_ref[3:4, :] = jnp.sum(st_ref[3], axis=0, keepdims=True) * inv_t
    out_ref[4:8, :] = jnp.zeros((4, R), jnp.float32)


def w_copy(wt_ref, wbuf, sems, seq, size):
    slot = seq % NB if isinstance(seq, int) else lax.rem(seq, NB)
    tile = seq % (NT + 1) if isinstance(seq, int) else lax.rem(seq, NT + 1)
    return pltpu.make_async_copy(wt_ref.at[pl.ds(tile * BV, size)], wbuf.at[slot, pl.ds(0, size)], sems.at[slot])


def w_start(wt_ref, wbuf, sems, seq, end):
    @pl.when((seq < end) & (seq != NT))
    def _():
        w_copy(wt_ref, wbuf, sems, seq, BV).start()

    @pl.when(seq == NT)
    def _():
        w_copy(wt_ref, wbuf, sems, seq, REM).start()


def head_loop(wt_ref, wbuf, wsem, x_ref, l_ref, st_ref, inv_t, ids, out=None, hooks=(), first=0, count=NT + 1,
              end=NT + 1, span=(0, R)):
    scale2 = inv_t * LOG2E
    if out is not None:
        o_ref, col0, stage, osem, out_inv_t, log_norm = out

    def out_copy(tile, size):
        slot = lax.rem(tile, 2) if not isinstance(tile, int) else tile % 2
        return pltpu.make_async_copy(stage.at[slot, pl.ds(0, size)],
                                     o_ref.at[pl.ds(tile * BV, size), pl.ds(col0, R)], osem.at[slot])

    def step(seq, size):
        last = isinstance(seq, int)
        slot = seq % NB if last else lax.rem(seq, NB)
        tile = seq - (NT + 1 if first > NT else 0)
        w_copy(wt_ref, wbuf, wsem, seq, size).wait()
        w_start(wt_ref, wbuf, wsem, jnp.int32(seq + NB - 1), end)
        fin = None
        if out is not None:
            if last:
                out_copy(tile - 2, BV).wait()
            else:
                @pl.when(tile >= 2)
                def _():
                    out_copy(tile - 2, BV).wait()
            fin = (stage.at[tile % 2 if last else lax.rem(tile, 2)], out_inv_t, log_norm)
        row0 = tile * BV if last else pl.multiple_of(tile * BV, BV)
        prev0 = row0 - BV if last else pl.multiple_of(jnp.maximum(row0 - BV, 0), BV)
        head_tile(wbuf.at[slot], x_ref, l_ref, st_ref, row0, size, prev0, scale2, ids, fin,
                  None if last else seq > first, span)
        if out is not None:
            out_copy(tile, size).start()

    def body(i, _):
        for at, hook in hooks:
            pl.when(i == at)(hook)
        step(i, BV)
        return 0

    stop = min(first + count, NT) if first <= NT else first + count
    lax.fori_loop(first, stop, body, 0)
    if first <= NT < first + count:
        step(NT, REM)
        row0, size = NT * BV, REM
    else:
        row0, size = (stop - 1) % (NT + 1) * BV, BV
    block_stats(l_ref, st_ref, row0, row0, size, scale2, ids, span=span)
    if out is not None:
        out_copy(NT - 1, BV).wait()
        out_copy(NT, REM).wait()


def place():
    a, b = lax.axis_index('tp2'), lax.axis_index('tp')
    return a, b // 2, b % 2


PEERS = [(i, j) for i in range(2) for j in range(4) if (i, j) != (0, 0)]


def peer(d):
    a, b = lax.axis_index('tp2'), lax.axis_index('tp')
    return {'tp2': (a + d[0]) % 2, 'tp': (b + d[1]) % 4}


def barrier():
    bar = pltpu.get_barrier_semaphore()
    for d in PEERS:
        pl.semaphore_signal(bar, inc=1, device_id=peer(d), device_id_type=MESH)
    pl.semaphore_wait(bar, 7)


def exchange(s_ref, res_ref, box, send_sem, recv_sem):
    copies = []
    for n, d in enumerate(PEERS):
        c = pltpu.make_async_remote_copy(s_ref, box.at[n], send_sem.at[n], recv_sem.at[n],
                                         device_id=peer(d), device_id_type=MESH)
        c.start()
        copies.append(c)
    for c in copies:
        c.wait()
    m = s_ref[0:1, :]
    for n in range(7):
        m = jnp.maximum(m, box[n, 0:1, :])
    k = jnp.exp(s_ref[0:1, :] - m)
    s, q, t = s_ref[1:2, :] * k, s_ref[2:3, :] * k, s_ref[3:4, :]
    for n in range(7):
        k = jnp.exp(box[n, 0:1, :] - m)
        s += box[n, 1:2, :] * k
        q += box[n, 2:3, :] * k
        t += box[n, 3:4, :]
    log_norm = m + jnp.log(s)
    res_ref[0:1, :] = log_norm
    res_ref[1:2, :] = log_norm - q / s
    res_ref[2:3, :] = t - log_norm
    res_ref[3:8, :] = jnp.zeros((5, R), jnp.float32)


def exchange_kernel(s_any, res_ref, box, send_sem, recv_sem, s_ref, s_sem):
    s_copy = pltpu.make_async_copy(s_any, s_ref, s_sem)
    s_copy.start()
    barrier()
    s_copy.wait()
    exchange(s_ref, res_ref, box, send_sem, recv_sem)


def first_kernel(h_ref, wg_ref, wu_ref, wd_ref, gain_ref, wt_ref, t_ref, ids_ref,
                 l_ref, x1_ref, res_ref,
                 wbuf, hbuf, hres, act, part, drecv, rbuf, x, st_ref, sbuf, box,
                 wsem, msem, hsem, hrsem, dsem, rsem, gsem, fsem, xsem, esem):
    y, xx, c = place()
    g = 2 * y + xx
    me = lax.axis_index('tp2') * 4 + lax.axis_index('tp')
    half = CH // 2
    own = half // 4

    def weights(n):
        src = (wg_ref, wu_ref)[n]
        return [pltpu.make_async_copy(src.at[pl.ds(k * 1024, 1024)], wbuf.at[n, :, pl.ds(k * 1024, 1024)],
                                      msem.at[2 * n + k]) for k in range(2)]

    down = pltpu.make_async_copy(wd_ref, wbuf.at[2], msem.at[4])

    def h_copy(q):
        return pltpu.make_async_copy(h_ref.at[pl.ds(q * CH, CH)], hbuf, hsem)

    def own_rows(q):
        return pl.ds(q * CH + c * half + g * own, own)

    def res_copy(q):
        return pltpu.make_async_copy(h_ref.at[own_rows(q)], hres.at[q], hrsem.at[q])

    def chip(d):
        cx = (xx + d % 2) % 2
        cy = (y + d // 2) % 2
        return cy, cx, {'tp2': cy, 'tp': 2 * cx + c}

    sibling = {'tp2': y, 'tp': 2 * xx + (c + 1) % 2}

    def d_copy(q):
        return pltpu.make_async_remote_copy(part.at[q, pl.ds(((c + 1) % 2) * half, half)], drecv.at[q],
                                            dsem.at[0, q], dsem.at[1, q], device_id=sibling, device_id_type=MESH)

    def r_copy(q, d):
        cy, cx, dev = chip(d)
        return pltpu.make_async_remote_copy(part.at[q, pl.ds(c * half + (2 * cy + cx) * own, own)], rbuf.at[q, d - 1],
                                            rsem.at[0, q, d - 1], rsem.at[1, q, d - 1], device_id=dev,
                                            device_id_type=MESH)

    def g_copy(q, d):
        return pltpu.make_async_remote_copy(x.at[own_rows(q)], x.at[own_rows(q)],
                                            gsem.at[0, q, d - 1], gsem.at[1, q, d - 1], device_id=chip(d)[2],
                                            device_id_type=MESH)

    def f_copy(q):
        rows = pl.ds(q * CH + c * half, half)
        return pltpu.make_async_remote_copy(x.at[rows], x.at[rows], fsem.at[0, q], fsem.at[1, q],
                                            device_id=sibling, device_id_type=MESH)

    def pair_sum(q):
        d_copy(q).wait()
        rows = pl.ds(c * half, half)
        part[q, rows, :] = (part[q, rows, :].astype(jnp.float32) + drecv[q].astype(jnp.float32)).astype(jnp.bfloat16)
        for d in (3, 1, 2):
            r_copy(q, d).start()

    def total(q):
        for d in (1, 2, 3):
            r_copy(q, d).wait()
        res_copy(q).wait()
        mlp = part[q, pl.ds(c * half + g * own, own), :].astype(jnp.float32)
        for d in range(3):
            mlp += rbuf[q, d].astype(jnp.float32)
        resid = hres[q].astype(jnp.float32) + mlp.astype(jnp.bfloat16).astype(jnp.float32)
        inv_rms = lax.rsqrt(jnp.mean(resid * resid, axis=-1, keepdims=True) + NORM_EPS)
        x[own_rows(q), :] = (gain_ref[...] * resid * inv_rms).astype(jnp.bfloat16)
        for d in (3, 1, 2):
            g_copy(q, d).start()

    def gathered(q):
        for d in (1, 2, 3):
            g_copy(q, d).wait()
        f_copy(q).start()

    h_copy(0).start()
    for n in range(2):
        for cp in weights(n):
            cp.start()
    down.start()
    for q in range(NQ):
        res_copy(q).start()
    init_stats(st_ref)
    barrier()

    def mlp(q, _):
        h_copy(q).wait()

        @pl.when(q == 0)
        def _():
            for n in range(2):
                for cp in weights(n):
                    cp.wait()
        h = hbuf
        for n in range(0, 1024, 512):
            pre = [jnp.dot(h[:, 0:1024], wbuf[k, :, n:n + 512], preferred_element_type=jnp.float32)
                   + jnp.dot(h[:, 1024:2048], wbuf[k, :, 1024 + n:1536 + n], preferred_element_type=jnp.float32)
                   for k in range(2)]
            act[:, n:n + 512] = (jax.nn.silu(pre[0]) * pre[1]).astype(jnp.bfloat16)

        @pl.when(q + 1 < NQ)
        def _():
            h_copy(q + 1).start()

        @pl.when(q == NQ - 1)
        def _():
            for t in range(NB - 1):
                w_copy(wt_ref, wbuf, wsem, t, BV).start()

        @pl.when(q == 0)
        def _():
            down.wait()

        @pl.when((q >= 1) & (q <= NQ // 2))
        def _():
            pair_sum(q - 1)
        for n in range(0, 2048, 512):
            part[q, :, n:n + 512] = jnp.dot(act[...], wbuf[2, :, n:n + 512],
                                            preferred_element_type=jnp.float32).astype(jnp.bfloat16)
        d_copy(q).start()

        @pl.when(q >= LAG)
        def _():
            total(q - LAG)
        return 0

    lax.fori_loop(0, NQ, mlp, 0)
    first, second, third = range(NQ // 4), range(NQ // 4, NQ // 2), range(NQ // 2, NQ)
    for q in range(NQ - LAG, NQ // 2):
        total(q)
    for q in first:
        gathered(q)
    for q in first:
        f_copy(q).wait()
    ids = ids_ref[:, 0:R] - me * V
    head = functools.partial(head_loop, wt_ref, wbuf, wsem, x.at[pl.ds(0, R)], l_ref, st_ref, 1.0 / t_ref[:, 0:R], ids,
                             end=NT + 1 + EARLY)
    head(first=0, count=EARLY, span=(0, R // 2))
    for q in second:
        gathered(q)
    for q in third:
        pair_sum(q)
    for q in second:
        f_copy(q).wait()

    def x1_copy():
        return pltpu.make_async_copy(x.at[pl.ds(R, R)], x1_ref, xsem)

    def last_rows():
        for q in third:
            f_copy(q).wait()
        x1_copy().start()

    hooks = [(EARLY + 1 + k, functools.partial(total, q)) for k, q in enumerate(third)]
    head(first=EARLY, count=NT + 1 - EARLY, hooks=hooks)
    for q in third:
        gathered(q)
    head(first=NT + 1, count=EARLY, span=(R // 2, R), hooks=[(NT + 1 + EARLY - 2, last_rows)])
    reduce_stats(st_ref, sbuf, 1.0 / t_ref[:, 0:R])
    x1_copy().wait()
    exchange(sbuf, res_ref, box, esem.at[0], esem.at[1])


def second_kernel(x_any, wt_ref, t_ref, ids_ref, res_ref, l_in, o_ref, l_ref, stat_ref,
                  wbuf, st_ref, wsem, stage, osem, x_ref, xsem):
    x_copy = pltpu.make_async_copy(x_any, x_ref, xsem)
    w_copy(wt_ref, wbuf, wsem, 0, BV).start()
    x_copy.start()
    for t in range(1, NB - 1):
        w_copy(wt_ref, wbuf, wsem, t, BV).start()
    init_stats(st_ref)
    x_copy.wait()
    me = lax.axis_index('tp2') * 4 + lax.axis_index('tp')
    ids = ids_ref[:, R:2 * R] - me * V
    head_loop(wt_ref, wbuf, wsem, x_ref, l_ref, st_ref, 1.0 / t_ref[:, R:2 * R], ids,
              out=(o_ref, 0, stage, osem, 1.0 / t_ref[:, 0:R], res_ref[0:1, :]))
    reduce_stats(st_ref, stat_ref, 1.0 / t_ref[:, R:2 * R])


def finish_kernel(l_ref, r0_ref, r1_ref, t_ref, o_in, o_ref, ln_ref, en_ref, tl_ref, stage, osem):
    for half, r in ((0, r0_ref), (1, r1_ref)):
        cols = slice(half * R, (half + 1) * R)
        ln_ref[:, cols] = r[0:1, :]
        en_ref[:, cols] = r[1:2, :]
        tl_ref[:, cols] = r[2:3, :]
    log_norm = r1_ref[0:1, :]
    inv_t = 1.0 / t_ref[:, R:2 * R]

    def out_copy(tile, size):
        slot = tile % FS if isinstance(tile, int) else lax.rem(tile, FS)
        return pltpu.make_async_copy(stage.at[slot, pl.ds(0, size)],
                                     o_ref.at[pl.ds(tile * FV, size), pl.ds(R, R)], osem.at[slot])

    def step(tile, size):
        slot = tile % FS if isinstance(tile, int) else lax.rem(tile, FS)
        if isinstance(tile, int):
            out_copy(tile - FS, FV).wait()
        else:
            @pl.when(tile >= FS)
            def _():
                out_copy(tile - FS, FV).wait()
        row0 = tile * FV if isinstance(tile, int) else pl.multiple_of(tile * FV, FV)
        stage[slot, 0:size, :] = (l_ref[pl.ds(row0, size), :] * inv_t - log_norm).astype(jnp.bfloat16)
        out_copy(tile, size).start()

    def body(i, _):
        step(i, FV)
        return 0

    n = V // FV
    lax.fori_loop(0, n, body, 0)
    step(n, V - n * FV)
    for t in range(n + 1 - FS, n):
        out_copy(t, FV).wait()
    out_copy(n, V - n * FV).wait()


def vspec():
    return pl.BlockSpec(memory_space=VM)


def aspec():
    return pl.BlockSpec(memory_space=pl.ANY)


def in_vmem(x):
    return pltpu.with_memory_space_constraint(x, VM)


def params(limit, **kw):
    return pltpu.CompilerParams(has_side_effects=True, vmem_limit_bytes=limit, **kw)


L_TYPE = VM((V, R), jnp.float32)
HEAD_COST = pl.CostEstimate(flops=2 * V * R * 2048, bytes_accessed=V * 4096, transcendentals=V * R)


def first_call(hidden, w_gate, w_up, w_down, gain, wt, temp, ids):
    dma = pltpu.SemaphoreType.DMA
    half, own = CH // 2, CH // 8
    return pl.pallas_call(
        first_kernel,
        out_shape=(L_TYPE, jax.ShapeDtypeStruct((R, 2048), jnp.bfloat16), jax.ShapeDtypeStruct((8, R), jnp.float32)),
        in_specs=[aspec()] * 4 + [vspec(), aspec(), vspec(), vspec()], out_specs=(vspec(), aspec(), vspec()),
        scratch_shapes=[
            VM((NB, BV, 2048), jnp.bfloat16), VM((CH, 2048), jnp.bfloat16), VM((NQ, own, 2048), jnp.bfloat16),
            VM((CH, 1024), jnp.bfloat16), VM((NQ, CH, 2048), jnp.bfloat16), VM((NQ, half, 2048), jnp.bfloat16),
            VM((NQ, 3, own, 2048), jnp.bfloat16), VM((2 * R, 2048), jnp.bfloat16), VM((4, 8, R), jnp.float32),
            VM((8, R), jnp.float32), VM((7, 8, R), jnp.float32),
            dma((NB,)), dma((5,)), dma, dma((NQ,)), dma((2, NQ)), dma((2, NQ, 3)), dma((2, NQ, 3)), dma((2, NQ)),
            dma, dma((2, 7))],
        name='first', cost_estimate=HEAD_COST,
        compiler_params=params(FIRST_LIMIT, collective_id=0))(hidden, w_gate, w_up, w_down, gain, wt, temp, ids)


def second_call(x1, wt, temp, ids, res, logits):
    return pl.pallas_call(
        second_kernel,
        out_shape=(jax.ShapeDtypeStruct((V, 2 * R), jnp.bfloat16), L_TYPE, jax.ShapeDtypeStruct((8, R), jnp.float32)),
        in_specs=[aspec(), aspec(), vspec(), vspec(), vspec(), vspec()], out_specs=(aspec(), vspec(), vspec()),
        scratch_shapes=[VM((NB, BV, 2048), jnp.bfloat16), VM((4, 8, R), jnp.float32), pltpu.SemaphoreType.DMA((NB,)),
                        VM((2, BV, R), jnp.bfloat16), pltpu.SemaphoreType.DMA((2,)),
                        VM((R, 2048), jnp.bfloat16), pltpu.SemaphoreType.DMA],
        input_output_aliases={5: 1}, name='second', cost_estimate=HEAD_COST,
        compiler_params=params(LIMIT))(x1, wt, temp, ids, res, in_vmem(logits))


def exchange_call(stats, cid):
    return pl.pallas_call(
        exchange_kernel, out_shape=jax.ShapeDtypeStruct((8, R), jnp.float32), in_specs=[aspec()], out_specs=vspec(),
        scratch_shapes=[VM((7, 8, R), jnp.float32), pltpu.SemaphoreType.DMA((7,)), pltpu.SemaphoreType.DMA((7,)),
                        VM((8, R), jnp.float32), pltpu.SemaphoreType.DMA],
        name='exchange%d' % cid, compiler_params=params(LIMIT, collective_id=cid))(
            pltpu.with_memory_space_constraint(stats, pltpu.HBM))


def finish_call(logits, r0, r1, temp, out):
    row = jax.ShapeDtypeStruct((1, 2 * R), jnp.float32)
    return pl.pallas_call(
        finish_kernel, out_shape=(jax.ShapeDtypeStruct((V, 2 * R), jnp.bfloat16), row, row, row),
        in_specs=[vspec(), vspec(), vspec(), vspec(), aspec()], out_specs=(aspec(), vspec(), vspec(), vspec()),
        scratch_shapes=[VM((FS, FV, R), jnp.bfloat16), pltpu.SemaphoreType.DMA((FS,))],
        input_output_aliases={4: 0}, name='finish', compiler_params=params(LIMIT))(in_vmem(logits), r0, r1, temp, out)


def solution(mesh):
    model_axes = ('tp2', 'tp')

    def local_step(hidden, w_gate, w_up, w_down, norm_gain, w_vocab, temperature, target_ids):
        temp = temperature.reshape(1, 2 * R)
        ids = target_ids.reshape(1, 2 * R)
        wt = w_vocab.T
        l0, x1, r0 = first_call(hidden, w_gate, w_up, w_down, norm_gain.reshape(1, -1), wt, temp, ids)
        out, l1, s1 = second_call(x1, wt, temp, ids, r0, l0)
        r1 = exchange_call(s1, 2)
        out, ln, en, tl = finish_call(l1, r0, r1, temp, out)
        return ln.reshape(-1), en.reshape(-1), tl.reshape(-1), out.T

    return jax.shard_map(
        local_step, mesh=mesh,
        in_specs=(P('dp', None), P(None, model_axes), P(None, model_axes), P(model_axes, None),
                  P(None), P(None, model_axes), P('dp'), P('dp')),
        out_specs=(P('dp'), P('dp'), P('dp'), P('dp', model_axes)),
        check_vma=False)
```

```python
import functools

import jax
import jax.numpy as jnp
from jax import lax
from jax.experimental import pallas as pl
from jax.experimental.pallas import tpu as pltpu
from jax.sharding import PartitionSpec as P

NORM_EPS = 1e-6
VM = pltpu.VMEM
MESH = pl.DeviceIdType.MESH
V = 16032
R = 512
BV = 1024
NT = V // BV
REM = V - NT * BV
SB = 512
SLICE = 128
NB = 3
CH = 128
NQ = 8
LAG = 4
EARLY = 8
FV, FS = 512, 8
MIB = 2 ** 20
LOG2E = 1.4426950408889634
FIRST_LIMIT = 31 * MIB
LIMIT = 26 * MIB


def block_stats(l_ref, st_ref, row0, vocab0, sb, scale2, ids, valid=None, span=(0, R)):
    for c in range(span[0], span[1], 128):
        lanes = slice(c, c + 128)
        a = scale2[:, lanes]
        m_old, s_old, q_old, t_old = (st_ref[n, :, lanes] for n in range(4))
        m, s, q, t = m_old, s_old, q_old, t_old
        rel = ids[:, lanes] - vocab0 - lax.broadcasted_iota(jnp.int32, (8, 128), 0)
        for r in range(0, sb, SLICE):
            n = min(SLICE, sb - r) // 8
            l3 = l_ref[pl.ds(row0 + r, n * 8), lanes].reshape(n, 8, 128)
            m_new = jnp.maximum(m, jnp.max(l3, axis=0))
            scale = jnp.exp2((m - m_new) * a)
            e = jnp.exp2((l3 - m_new[None]) * a[None])
            s = s * scale + jnp.sum(e, axis=0)
            q = q * scale + jnp.sum(e * l3, axis=0)
            for j in range(n):
                t = jnp.where(rel == r + 8 * j, l3[j], t)
            m = m_new
        if valid is not None:
            m, s = jnp.where(valid, m, m_old), jnp.where(valid, s, s_old)
            q, t = jnp.where(valid, q, q_old), jnp.where(valid, t, t_old)
        st_ref[0, :, lanes], st_ref[1, :, lanes], st_ref[2, :, lanes], st_ref[3, :, lanes] = m, s, q, t


def head_tile(w_ref, x_ref, l_ref, st_ref, row0, bv, prev0, scale2, ids, fin=None, valid=None, span=(0, R)):
    def stats(off, n):
        block_stats(l_ref, st_ref, prev0 + off, prev0 + off, n, scale2, ids, valid, span)

    def dot(off, n):
        sb = min(n, bv - off)
        if sb <= 0:
            return
        rows = pl.ds(row0 + off, sb)
        if fin is not None:
            stage, inv_t, log_norm = fin
            stage[pl.ds(off, sb), :] = (l_ref[rows, :] * inv_t - log_norm).astype(jnp.bfloat16)
        l_ref[rows, span[0]:span[1]] = lax.dot_general(w_ref[pl.ds(off, sb), :], x_ref[span[0]:span[1], :],
                                                       (((1,), (1,)), ((), ())), preferred_element_type=jnp.float32)

    if fin is not None:
        dot(0, SB)
        stats(0, BV)
        dot(SB, SB)
    else:
        for off in range(0, BV, SB // 2):
            stats(off, SB // 2)
            dot(off, SB // 2)


def init_stats(st_ref):
    st_ref[0] = jnp.full((8, R), -3.0e38, jnp.float32)
    st_ref[1] = jnp.zeros((8, R), jnp.float32)
    st_ref[2] = jnp.zeros((8, R), jnp.float32)
    st_ref[3] = jnp.zeros((8, R), jnp.float32)


def reduce_stats(st_ref, out_ref, inv_t):
    m = jnp.max(st_ref[0], axis=0, keepdims=True)
    scale = jnp.exp2((st_ref[0] - m) * (inv_t * LOG2E))
    out_ref[0:1, :] = m * inv_t
    out_ref[1:2, :] = jnp.sum(st_ref[1] * scale, axis=0, keepdims=True)
    out_ref[2:3, :] = jnp.sum(st_ref[2] * scale, axis=0, keepdims=True) * inv_t
    out_ref[3:4, :] = jnp.sum(st_ref[3], axis=0, keepdims=True) * inv_t
    out_ref[4:8, :] = jnp.zeros((4, R), jnp.float32)


def w_copy(wt_ref, wbuf, sems, seq, size):
    slot = seq % NB if isinstance(seq, int) else lax.rem(seq, NB)
    tile = seq % (NT + 1) if isinstance(seq, int) else lax.rem(seq, NT + 1)
    return pltpu.make_async_copy(wt_ref.at[pl.ds(tile * BV, size)], wbuf.at[slot, pl.ds(0, size)], sems.at[slot])


def w_start(wt_ref, wbuf, sems, seq, end):
    @pl.when((seq < end) & (seq != NT))
    def _():
        w_copy(wt_ref, wbuf, sems, seq, BV).start()

    @pl.when(seq == NT)
    def _():
        w_copy(wt_ref, wbuf, sems, seq, REM).start()


def head_loop(wt_ref, wbuf, wsem, x_ref, l_ref, st_ref, inv_t, ids, out=None, hooks=(), first=0, count=NT + 1,
              end=NT + 1, span=(0, R)):
    scale2 = inv_t * LOG2E
    if out is not None:
        o_ref, col0, stage, osem, out_inv_t, log_norm = out

    def out_copy(tile, size):
        slot = lax.rem(tile, 2) if not isinstance(tile, int) else tile % 2
        return pltpu.make_async_copy(stage.at[slot, pl.ds(0, size)],
                                     o_ref.at[pl.ds(tile * BV, size), pl.ds(col0, R)], osem.at[slot])

    def step(seq, size):
        last = isinstance(seq, int)
        slot = seq % NB if last else lax.rem(seq, NB)
        tile = seq - (NT + 1 if first > NT else 0)
        w_copy(wt_ref, wbuf, wsem, seq, size).wait()
        w_start(wt_ref, wbuf, wsem, jnp.int32(seq + NB - 1), end)
        fin = None
        if out is not None:
            if last:
                out_copy(tile - 2, BV).wait()
            else:
                @pl.when(tile >= 2)
                def _():
                    out_copy(tile - 2, BV).wait()
            fin = (stage.at[tile % 2 if last else lax.rem(tile, 2)], out_inv_t, log_norm)
        row0 = tile * BV if last else pl.multiple_of(tile * BV, BV)
        prev0 = row0 - BV if last else pl.multiple_of(jnp.maximum(row0 - BV, 0), BV)
        head_tile(wbuf.at[slot], x_ref, l_ref, st_ref, row0, size, prev0, scale2, ids, fin,
                  None if last else seq > first, span)
        if out is not None:
            out_copy(tile, size).start()

    def body(i, _):
        for at, hook in hooks:
            pl.when(i == at)(hook)
        step(i, BV)
        return 0

    stop = min(first + count, NT) if first <= NT else first + count
    lax.fori_loop(first, stop, body, 0)
    if first <= NT < first + count:
        step(NT, REM)
        row0, size = NT * BV, REM
    else:
        row0, size = (stop - 1) % (NT + 1) * BV, BV
    block_stats(l_ref, st_ref, row0, row0, size, scale2, ids, span=span)
    if out is not None:
        out_copy(NT - 1, BV).wait()
        out_copy(NT, REM).wait()


def place():
    a, b = lax.axis_index('tp2'), lax.axis_index('tp')
    return a, b // 2, b % 2


PEERS = [(i, j) for i in range(2) for j in range(4) if (i, j) != (0, 0)]


def peer(d):
    a, b = lax.axis_index('tp2'), lax.axis_index('tp')
    return {'tp2': (a + d[0]) % 2, 'tp': (b + d[1]) % 4}


def barrier():
    bar = pltpu.get_barrier_semaphore()
    for d in PEERS:
        pl.semaphore_signal(bar, inc=1, device_id=peer(d), device_id_type=MESH)
    pl.semaphore_wait(bar, 7)


def exchange(s_ref, res_ref, box, send_sem, recv_sem):
    copies = []
    for n, d in enumerate(PEERS):
        c = pltpu.make_async_remote_copy(s_ref, box.at[n], send_sem.at[n], recv_sem.at[n],
                                         device_id=peer(d), device_id_type=MESH)
        c.start()
        copies.append(c)
    for c in copies:
        c.wait()
    m = s_ref[0:1, :]
    for n in range(7):
        m = jnp.maximum(m, box[n, 0:1, :])
    k = jnp.exp(s_ref[0:1, :] - m)
    s, q, t = s_ref[1:2, :] * k, s_ref[2:3, :] * k, s_ref[3:4, :]
    for n in range(7):
        k = jnp.exp(box[n, 0:1, :] - m)
        s += box[n, 1:2, :] * k
        q += box[n, 2:3, :] * k
        t += box[n, 3:4, :]
    log_norm = m + jnp.log(s)
    res_ref[0:1, :] = log_norm
    res_ref[1:2, :] = log_norm - q / s
    res_ref[2:3, :] = t - log_norm
    res_ref[3:8, :] = jnp.zeros((5, R), jnp.float32)


def exchange_kernel(s_any, res_ref, box, send_sem, recv_sem, s_ref, s_sem):
    s_copy = pltpu.make_async_copy(s_any, s_ref, s_sem)
    s_copy.start()
    barrier()
    s_copy.wait()
    exchange(s_ref, res_ref, box, send_sem, recv_sem)


def first_kernel(h_ref, wg_ref, wu_ref, wd_ref, gain_ref, wt_ref, t_ref, ids_ref,
                 l_ref, x1_ref, res_ref,
                 wbuf, hbuf, hres, act, part, drecv, rbuf, x, st_ref, sbuf, box,
                 wsem, msem, hsem, hrsem, dsem, rsem, gsem, fsem, xsem, esem):
    y, xx, c = place()
    g = 2 * y + xx
    me = lax.axis_index('tp2') * 4 + lax.axis_index('tp')
    half = CH // 2
    own = half // 4

    def weights(n):
        src = (wg_ref, wu_ref)[n]
        return [pltpu.make_async_copy(src.at[pl.ds(k * 1024, 1024)], wbuf.at[n, :, pl.ds(k * 1024, 1024)],
                                      msem.at[2 * n + k]) for k in range(2)]

    down = pltpu.make_async_copy(wd_ref, wbuf.at[2], msem.at[4])

    def h_copy(q):
        return pltpu.make_async_copy(h_ref.at[pl.ds(q * CH, CH)], hbuf, hsem)

    def own_rows(q):
        return pl.ds(q * CH + c * half + g * own, own)

    def res_copy(q):
        return pltpu.make_async_copy(h_ref.at[own_rows(q)], hres.at[q], hrsem.at[q])

    def chip(d):
        cx = (xx + d % 2) % 2
        cy = (y + d // 2) % 2
        return cy, cx, {'tp2': cy, 'tp': 2 * cx + c}

    sibling = {'tp2': y, 'tp': 2 * xx + (c + 1) % 2}

    def d_copy(q):
        return pltpu.make_async_remote_copy(part.at[q, pl.ds(((c + 1) % 2) * half, half)], drecv.at[q],
                                            dsem.at[0, q], dsem.at[1, q], device_id=sibling, device_id_type=MESH)

    def r_copy(q, d):
        cy, cx, dev = chip(d)
        return pltpu.make_async_remote_copy(part.at[q, pl.ds(c * half + (2 * cy + cx) * own, own)], rbuf.at[q, d - 1],
                                            rsem.at[0, q, d - 1], rsem.at[1, q, d - 1], device_id=dev,
                                            device_id_type=MESH)

    def g_copy(q, d):
        return pltpu.make_async_remote_copy(x.at[own_rows(q)], x.at[own_rows(q)],
                                            gsem.at[0, q, d - 1], gsem.at[1, q, d - 1], device_id=chip(d)[2],
                                            device_id_type=MESH)

    def f_copy(q):
        rows = pl.ds(q * CH + c * half, half)
        return pltpu.make_async_remote_copy(x.at[rows], x.at[rows], fsem.at[0, q], fsem.at[1, q],
                                            device_id=sibling, device_id_type=MESH)

    def pair_sum(q):
        d_copy(q).wait()
        rows = pl.ds(c * half, half)
        part[q, rows, :] = (part[q, rows, :].astype(jnp.float32) + drecv[q].astype(jnp.float32)).astype(jnp.bfloat16)
        for d in (3, 1, 2):
            r_copy(q, d).start()

    def total(q):
        for d in (1, 2, 3):
            r_copy(q, d).wait()
        res_copy(q).wait()
        mlp = part[q, pl.ds(c * half + g * own, own), :].astype(jnp.float32)
        for d in range(3):
            mlp += rbuf[q, d].astype(jnp.float32)
        resid = hres[q].astype(jnp.float32) + mlp.astype(jnp.bfloat16).astype(jnp.float32)
        inv_rms = lax.rsqrt(jnp.mean(resid * resid, axis=-1, keepdims=True) + NORM_EPS)
        x[own_rows(q), :] = (gain_ref[...] * resid * inv_rms).astype(jnp.bfloat16)
        for d in (3, 1, 2):
            g_copy(q, d).start()

    def gathered(q):
        for d in (1, 2, 3):
            g_copy(q, d).wait()
        f_copy(q).start()

    h_copy(0).start()
    for n in range(2):
        for cp in weights(n):
            cp.start()
    down.start()
    for q in range(NQ):
        res_copy(q).start()
    init_stats(st_ref)
    barrier()

    def mlp(q, _):
        h_copy(q).wait()

        @pl.when(q == 0)
        def _():
            for n in range(2):
                for cp in weights(n):
                    cp.wait()
        h = hbuf
        for n in range(0, 1024, 512):
            pre = [jnp.dot(h[:, 0:1024], wbuf[k, :, n:n + 512], preferred_element_type=jnp.float32)
                   + jnp.dot(h[:, 1024:2048], wbuf[k, :, 1024 + n:1536 + n], preferred_element_type=jnp.float32)
                   for k in range(2)]
            act[:, n:n + 512] = (jax.nn.silu(pre[0]) * pre[1]).astype(jnp.bfloat16)

        @pl.when(q + 1 < NQ)
        def _():
            h_copy(q + 1).start()

        @pl.when(q == NQ - 1)
        def _():
            for t in range(NB - 1):
                w_copy(wt_ref, wbuf, wsem, t, BV).start()

        @pl.when(q == 0)
        def _():
            down.wait()

        @pl.when((q >= 1) & (q <= NQ // 2))
        def _():
            pair_sum(q - 1)
        for n in range(0, 2048, 512):
            part[q, :, n:n + 512] = jnp.dot(act[...], wbuf[2, :, n:n + 512],
                                            preferred_element_type=jnp.float32).astype(jnp.bfloat16)
        d_copy(q).start()

        @pl.when(q >= LAG)
        def _():
            total(q - LAG)
        return 0

    lax.fori_loop(0, NQ, mlp, 0)
    first, second, third = range(NQ // 4), range(NQ // 4, NQ // 2), range(NQ // 2, NQ)
    for q in range(NQ - LAG, NQ // 2):
        total(q)
    for q in first:
        gathered(q)
    for q in first:
        f_copy(q).wait()
    ids = ids_ref[:, 0:R] - me * V
    head = functools.partial(head_loop, wt_ref, wbuf, wsem, x.at[pl.ds(0, R)], l_ref, st_ref, 1.0 / t_ref[:, 0:R], ids,
                             end=NT + 1 + EARLY)
    head(first=0, count=EARLY, span=(0, R // 2))
    for q in second:
        gathered(q)
    for q in third:
        pair_sum(q)
    for q in second:
        f_copy(q).wait()

    def x1_copy():
        return pltpu.make_async_copy(x.at[pl.ds(R, R)], x1_ref, xsem)

    def last_rows():
        for q in third:
            f_copy(q).wait()
        x1_copy().start()

    hooks = [(EARLY + 2 + k, functools.partial(total, q)) for k, q in enumerate(third)]
    head(first=EARLY, count=NT + 1 - EARLY, hooks=hooks)
    for q in third:
        gathered(q)
    head(first=NT + 1, count=EARLY, span=(R // 2, R), hooks=[(NT + 1 + EARLY - 2, last_rows)])
    reduce_stats(st_ref, sbuf, 1.0 / t_ref[:, 0:R])
    x1_copy().wait()
    exchange(sbuf, res_ref, box, esem.at[0], esem.at[1])


def second_kernel(x_any, wt_ref, t_ref, ids_ref, res_ref, l_in, o_ref, l_ref, stat_ref,
                  wbuf, st_ref, wsem, stage, osem, x_ref, xsem):
    x_copy = pltpu.make_async_copy(x_any, x_ref, xsem)
    w_copy(wt_ref, wbuf, wsem, 0, BV).start()
    x_copy.start()
    for t in range(1, NB - 1):
        w_copy(wt_ref, wbuf, wsem, t, BV).start()
    init_stats(st_ref)
    x_copy.wait()
    me = lax.axis_index('tp2') * 4 + lax.axis_index('tp')
    ids = ids_ref[:, R:2 * R] - me * V
    head_loop(wt_ref, wbuf, wsem, x_ref, l_ref, st_ref, 1.0 / t_ref[:, R:2 * R], ids,
              out=(o_ref, 0, stage, osem, 1.0 / t_ref[:, 0:R], res_ref[0:1, :]))
    reduce_stats(st_ref, stat_ref, 1.0 / t_ref[:, R:2 * R])


def finish_kernel(l_ref, r0_ref, r1_ref, t_ref, o_in, o_ref, ln_ref, en_ref, tl_ref, stage, osem):
    for half, r in ((0, r0_ref), (1, r1_ref)):
        cols = slice(half * R, (half + 1) * R)
        ln_ref[:, cols] = r[0:1, :]
        en_ref[:, cols] = r[1:2, :]
        tl_ref[:, cols] = r[2:3, :]
    log_norm = r1_ref[0:1, :]
    inv_t = 1.0 / t_ref[:, R:2 * R]

    def out_copy(tile, size):
        slot = tile % FS if isinstance(tile, int) else lax.rem(tile, FS)
        return pltpu.make_async_copy(stage.at[slot, pl.ds(0, size)],
                                     o_ref.at[pl.ds(tile * FV, size), pl.ds(R, R)], osem.at[slot])

    def step(tile, size):
        slot = tile % FS if isinstance(tile, int) else lax.rem(tile, FS)
        if isinstance(tile, int):
            out_copy(tile - FS, FV).wait()
        else:
            @pl.when(tile >= FS)
            def _():
                out_copy(tile - FS, FV).wait()
        row0 = tile * FV if isinstance(tile, int) else pl.multiple_of(tile * FV, FV)
        stage[slot, 0:size, :] = (l_ref[pl.ds(row0, size), :] * inv_t - log_norm).astype(jnp.bfloat16)
        out_copy(tile, size).start()

    def body(i, _):
        step(i, FV)
        return 0

    n = V // FV
    lax.fori_loop(0, n, body, 0)
    step(n, V - n * FV)
    for t in range(n + 1 - FS, n):
        out_copy(t, FV).wait()
    out_copy(n, V - n * FV).wait()


def vspec():
    return pl.BlockSpec(memory_space=VM)


def aspec():
    return pl.BlockSpec(memory_space=pl.ANY)


def in_vmem(x):
    return pltpu.with_memory_space_constraint(x, VM)


def params(limit, **kw):
    return pltpu.CompilerParams(has_side_effects=True, vmem_limit_bytes=limit, **kw)


L_TYPE = VM((V, R), jnp.float32)
HEAD_COST = pl.CostEstimate(flops=2 * V * R * 2048, bytes_accessed=V * 4096, transcendentals=V * R)


def first_call(hidden, w_gate, w_up, w_down, gain, wt, temp, ids):
    dma = pltpu.SemaphoreType.DMA
    half, own = CH // 2, CH // 8
    return pl.pallas_call(
        first_kernel,
        out_shape=(L_TYPE, jax.ShapeDtypeStruct((R, 2048), jnp.bfloat16), jax.ShapeDtypeStruct((8, R), jnp.float32)),
        in_specs=[aspec()] * 4 + [vspec(), aspec(), vspec(), vspec()], out_specs=(vspec(), aspec(), vspec()),
        scratch_shapes=[
            VM((NB, BV, 2048), jnp.bfloat16), VM((CH, 2048), jnp.bfloat16), VM((NQ, own, 2048), jnp.bfloat16),
            VM((CH, 1024), jnp.bfloat16), VM((NQ, CH, 2048), jnp.bfloat16), VM((NQ, half, 2048), jnp.bfloat16),
            VM((NQ, 3, own, 2048), jnp.bfloat16), VM((2 * R, 2048), jnp.bfloat16), VM((4, 8, R), jnp.float32),
            VM((8, R), jnp.float32), VM((7, 8, R), jnp.float32),
            dma((NB,)), dma((5,)), dma, dma((NQ,)), dma((2, NQ)), dma((2, NQ, 3)), dma((2, NQ, 3)), dma((2, NQ)),
            dma, dma((2, 7))],
        name='first', cost_estimate=HEAD_COST,
        compiler_params=params(FIRST_LIMIT, collective_id=0))(hidden, w_gate, w_up, w_down, gain, wt, temp, ids)


def second_call(x1, wt, temp, ids, res, logits):
    return pl.pallas_call(
        second_kernel,
        out_shape=(jax.ShapeDtypeStruct((V, 2 * R), jnp.bfloat16), L_TYPE, jax.ShapeDtypeStruct((8, R), jnp.float32)),
        in_specs=[aspec(), aspec(), vspec(), vspec(), vspec(), vspec()], out_specs=(aspec(), vspec(), vspec()),
        scratch_shapes=[VM((NB, BV, 2048), jnp.bfloat16), VM((4, 8, R), jnp.float32), pltpu.SemaphoreType.DMA((NB,)),
                        VM((2, BV, R), jnp.bfloat16), pltpu.SemaphoreType.DMA((2,)),
                        VM((R, 2048), jnp.bfloat16), pltpu.SemaphoreType.DMA],
        input_output_aliases={5: 1}, name='second', cost_estimate=HEAD_COST,
        compiler_params=params(LIMIT))(x1, wt, temp, ids, res, in_vmem(logits))


def exchange_call(stats, cid):
    return pl.pallas_call(
        exchange_kernel, out_shape=jax.ShapeDtypeStruct((8, R), jnp.float32), in_specs=[aspec()], out_specs=vspec(),
        scratch_shapes=[VM((7, 8, R), jnp.float32), pltpu.SemaphoreType.DMA((7,)), pltpu.SemaphoreType.DMA((7,)),
                        VM((8, R), jnp.float32), pltpu.SemaphoreType.DMA],
        name='exchange%d' % cid, compiler_params=params(LIMIT, collective_id=cid))(
            pltpu.with_memory_space_constraint(stats, pltpu.HBM))


def finish_call(logits, r0, r1, temp, out):
    row = jax.ShapeDtypeStruct((1, 2 * R), jnp.float32)
    return pl.pallas_call(
        finish_kernel, out_shape=(jax.ShapeDtypeStruct((V, 2 * R), jnp.bfloat16), row, row, row),
        in_specs=[vspec(), vspec(), vspec(), vspec(), aspec()], out_specs=(aspec(), vspec(), vspec(), vspec()),
        scratch_shapes=[VM((FS, FV, R), jnp.bfloat16), pltpu.SemaphoreType.DMA((FS,))],
        input_output_aliases={4: 0}, name='finish', compiler_params=params(LIMIT))(in_vmem(logits), r0, r1, temp, out)


def solution(mesh):
    model_axes = ('tp2', 'tp')

    def local_step(hidden, w_gate, w_up, w_down, norm_gain, w_vocab, temperature, target_ids):
        temp = temperature.reshape(1, 2 * R)
        ids = target_ids.reshape(1, 2 * R)
        wt = w_vocab.T
        l0, x1, r0 = first_call(hidden, w_gate, w_up, w_down, norm_gain.reshape(1, -1), wt, temp, ids)
        out, l1, s1 = second_call(x1, wt, temp, ids, r0, l0)
        r1 = exchange_call(s1, 2)
        out, ln, en, tl = finish_call(l1, r0, r1, temp, out)
        return ln.reshape(-1), en.reshape(-1), tl.reshape(-1), out.T

    return jax.shard_map(
        local_step, mesh=mesh,
        in_specs=(P('dp', None), P(None, model_axes), P(None, model_axes), P(model_axes, None),
                  P(None), P(None, model_axes), P('dp'), P('dp')),
        out_specs=(P('dp'), P('dp'), P('dp'), P('dp', model_axes)),
        check_vma=False)
```
